128 devices in a mesh: gx: 4 (over x), gy: 4 (over y_lo, core), gz: 8 (over z, y_hi).
Axes of the slice: x: 4, y: 4 (y_hi: 2, y_lo: 2; y = y_hi * 2 + y_lo), z: 4, core: 2. Of those that a mesh axis runs over, the one named last changes fastest.
Arguments:
- grad_bucket: bfloat16 [128, 1, 3584, 1024], P(('gx', 'gy', 'gz')), may hold values from -72000 to 72000
- parameters: bfloat16 [1, 3584, 1024], P(None, ('gx', 'gy', 'gz')), may hold values from -4 to 4
- row_state: float32 [1, 3584], P(None, ('gx', 'gy', 'gz')), may hold values from 0.01 to 10
- column_state: float32 [1, 1024], replicated, may hold values from 0.01 to 10
Outputs:
- new_parameters: bfloat16 [1, 3584, 1024], P(None, ('gx', 'gy', 'gz'))
- row_next: float32 [1, 3584], P(None, ('gx', 'gy', 'gz'))
- column_next: float32 [1, 1024], replicated
- first_layer: bfloat16 [3584, 1024], replicated
The draws below stay inside these ranges and needn't reach their ends.
All inputs are finite; a program needn't handle non-finite values.
Results may differ from the reference program's by a relative error of at most 0.011.
Values may be sent and summed in bfloat16 or wider, within the bound.
A program may use at most 128 MiB of HBM per device.

```python
import math
import jax
import jax.numpy as jnp
from jax import lax

D = 3584
LAYERS = 1
KW = 1024
DEVICES = 128


def draw_grad_bucket(key, part):
    row_key = jax.random.fold_in(key, 11)
    column_key = jax.random.fold_in(key, 12)
    owner_key = jax.random.fold_in(key, 13)
    row_index = jnp.arange(D, dtype=jnp.int32)
    rising = jnp.exp(math.log(3.0) * row_index.astype(jnp.float32) / (D - 1))
    row_scale = rising[None, :] * jnp.exp(math.log(10.0) * jax.random.uniform(row_key, (LAYERS, D)))
    column_scale = jnp.exp(math.log(10.0) * jax.random.uniform(column_key, (LAYERS, KW)))
    owners = jax.random.permutation(owner_key, DEVICES).astype(jnp.int32)
    row_owner = row_index // (D // DEVICES)

    def one_device(device):
        device_key = jax.random.fold_in(key, 1000 + device)
        noise_part = jnp.clip(jax.random.normal(device_key, (LAYERS, D, KW)), -6.0, 6.0)
        spiked = jnp.where(row_owner == owners[device], 24.0, 1.0)
        values = noise_part * row_scale[:, :, None] * column_scale[:, None, :] * spiked[None, :, None]
        return values.astype(jnp.bfloat16)
    return lax.map(one_device, jnp.arange(DEVICES, dtype=jnp.int32))


def steps_of(rng, dims, pieces, low, high):
    loudness, own = 1.0, jax.random.fold_in(rng, 6)
    for axis_at, shards_of in pieces:
        steps = jnp.exp(jax.random.uniform(jax.random.fold_in(own, axis_at), (shards_of,), jnp.float32, low / len(pieces), high / len(pieces)))
        loudness = loudness * jnp.repeat(steps, dims[axis_at] // shards_of).reshape([-1 if axis == axis_at else 1 for axis in range(len(dims))])
    return loudness


def normal_values(stream_key, extent, scale, most, shards=(), kind=jnp.bfloat16):
    array = scale * jax.random.normal(stream_key, extent, jnp.float32)
    if shards:
        array = array * steps_of(stream_key, extent, shards, -0.22, 0.18)
    return jnp.clip(array, -most, most).astype(kind)


def setup_inputs(seed: int = 0) -> dict:
    key_of = jax.random.split(jax.random.key(seed), 5)
    grad_bucket = draw_grad_bucket(jax.random.fold_in(key_of[4], 71), 0)
    parameters = normal_values(key_of[1], (LAYERS, D, KW), 1.0, 4.0, ((1, 128),))
    row_state = jnp.clip(jnp.exp(math.log(10.0) - 6.9077553 * jax.random.uniform(key_of[2], (LAYERS, D), jnp.float32) ** steps_of(key_of[2], (LAYERS, D), ((1, 128),), -0.2, 0.2)), 0.01, 10.0)
    column_state = jnp.clip(jnp.exp(jax.random.uniform(key_of[3], (LAYERS, KW), jnp.float32, math.log(0.01), math.log(10.0))), 0.01, 10.0)
    return dict(grad_bucket=grad_bucket, parameters=parameters, row_state=row_state, column_state=column_state)


beta_two = 0.8
step_size = 0.5

def reference(grad_bucket, parameters, row_state, column_state):

    def accumulate(running, device_grad):
        return (running + device_grad.astype(jnp.float32), None)
    summed, unused = lax.scan(accumulate, jnp.zeros((LAYERS, D, KW), jnp.float32), grad_bucket)
    norm_square = jnp.sum(summed * summed)
    clip_level = 0.5 * math.sqrt(LAYERS * D * KW)
    factor = jnp.minimum(jnp.float32(1.0), clip_level / jnp.sqrt(norm_square + 1e-06))
    clipped = factor * summed
    squares = clipped * clipped
    row_next = beta_two * row_state + (1.0 - beta_two) * lax.optimization_barrier(jnp.mean(squares, axis=2))
    column_next = beta_two * column_state + (1.0 - beta_two) * lax.optimization_barrier(jnp.mean(squares, axis=1))
    row_average = lax.optimization_barrier(jnp.mean(row_next, axis=1))
    second = row_next[:, :, None] * column_next[:, None, :] / row_average[:, None, None]
    update = clipped / jnp.sqrt(second)
    new_parameters = (parameters.astype(jnp.float32) - step_size * update).astype(jnp.bfloat16)
    return (new_parameters, row_next, column_next, new_parameters[0])
```

```python
import math

import jax
import jax.numpy as jnp
from jax import lax
from jax.experimental import pallas as pl
from jax.experimental.pallas import tpu as pltpu
from jax.sharding import PartitionSpec as P

D = 3584
KW = 1024
CLIP = 0.5 * math.sqrt(D * KW)
BETA = 0.8
STEP = 0.5
MESH = pl.DeviceIdType.MESH
F32 = jnp.float32
BF16 = jnp.bfloat16

ORDER = ("xyz", "yzx", "zxy")
STRIP = ((0, 24), (24, 40), (40, 56))
ROWS = tuple(56 + b - a for a, b in STRIP)
LD, PR, RLP, RLM, FM, FP, SE, TH = 0, 4, 8, 12, 16, 20, 24, 27
GT, GS, GM, GP, GO, GC = 30, 33, 36, 40, 44, 48
NRECV = 49
NSEND = 8


def mod4(v):
    return lax.rem(v, 4)


def where_am_i():
    gx, gy, gz = lax.axis_index("gx"), lax.axis_index("gy"), lax.axis_index("gz")
    lo, core = lax.div(gy, 2), lax.rem(gy, 2)
    z, hi = lax.div(gz, 2), lax.rem(gz, 2)
    return {"x": gx, "y": 2 * hi + lo, "z": z}, lo, hi, core


def device(at, core):
    return (at["x"], lax.rem(at["y"], 2) * 2 + core, at["z"] * 2 + lax.div(at["y"], 2))


def pieces(t, a1):
    every = slice(None)
    if t == 0:
        return [((a1, every, None, every), h, (pl.ds(2 * h, 2), every)) for h in (0, 1)]
    if t == 1:
        hi, lo = lax.div(a1, 2), lax.rem(a1, 2)
        return [((every, lo, None, z), hi, (z, every)) for z in range(4)]
    return [((every, every, None, a1), h, (every, pl.ds(2 * h, 2))) for h in (0, 1)]


def rectangles(t):
    return [(t, 0, 56, 0), (3, STRIP[t][0], STRIP[t][1], 56)]


def copies(t, a1, core, whole, part):
    out = []
    for (x, lo, _, z), h, (i, j) in pieces(t, a1):
        for tile, r0, r1, d0 in rectangles(t):
            col = h * 512 + tile * 128
            if not isinstance(col, int):
                col = pl.multiple_of(col, 128)
            out.append((
                whole.at[x, lo, core, z, pl.ds(r0, r1 - r0), pl.ds(col, 128)],
                part.at[a1, i, j, pl.ds(d0, r1 - r0), :],
            ))
    return out


def step_kernel(*refs):
    (g, par_in, rs_in, cs_in), refs = refs[:4], refs[4:]
    outs, refs = refs[:9], refs[9:]
    own, other = outs[0:3], outs[3:6]
    newp, rown, coln = outs[6:9]
    it = iter(refs)
    take3 = lambda: [next(it) for _ in range(3)]
    w, pr, rlp, rlm, fm, fp, s1, r2, s2, r3, s3 = (take3() for _ in range(11))
    par, line, rs, cs, pf, px, pxr, rx, rxr, rq, rqr, st1, st2, st3 = (next(it) for _ in range(14))
    recv, send, xr, xs, t1r, t1s, t2r, t2s, near = (next(it) for _ in range(9))

    at, lo, hi, core = where_am_i()

    def moved(axis, k):
        to = dict(at)
        to[axis] = mod4(at[axis] + k)
        return to

    def push(src, dst, ssem, rsem, to, tc):
        pltpu.make_async_remote_copy(
            src_ref=src, dst_ref=dst, send_sem=ssem, recv_sem=rsem, device_id=device(to, tc), device_id_type=MESH
        ).start()

    def settle(ref, sem):
        pltpu.make_async_copy(ref, ref, sem).wait()

    axes = [tuple(ORDER[t]) for t in range(3)]
    pos = [tuple(at[a] for a in axes[t]) for t in range(3)]

    def rel(t, level, k):
        return mod4(pos[t][level] + k)

    small = ((par_in, par), (rs_in, line), (cs_in, cs))
    for i, (src, dst) in enumerate(small):
        pltpu.make_async_copy(src, dst, near.at[i]).start()
    for k in (2, 1, 3, 0):
        for t in range(3):
            for src, dst in copies(t, rel(t, 0, k), core, g, w[t]):
                pltpu.make_async_copy(src, dst, recv.at[t, LD + k]).start()

    barrier = pltpu.get_barrier_semaphore()
    for axis in "xyz":
        for k in (1, 2, 3):
            pl.semaphore_signal(barrier, inc=1, device_id=device(moved(axis, k), core), device_id_type=MESH)
    for k in range(4):
        pl.semaphore_signal(barrier, inc=1, device_id=device(moved("x", k), 1 - core), device_id_type=MESH)
    pl.semaphore_wait(barrier, 13)

    for k in (2, 1, 3, 0):
        for t in range(3):
            for src, (_, dst) in zip(
                [s for s, _ in copies(t, rel(t, 0, k), 1 - core, g, pr[t])], copies(t, rel(t, 0, k), core, g, pr[t])
            ):
                push(src, dst, send.at[t, 0], recv.at[t, PR + k], at, 1 - core)

    pf[...] = jnp.zeros_like(pf)
    for i, (src, dst) in enumerate(small):
        pltpu.make_async_copy(src, dst, near.at[i]).wait()
    wide = par[...].astype(F32)

    @pl.when(hi == 0)
    def _():
        pf[0:28, :] = wide

    @pl.when(hi == 1)
    def _():
        pf[28:56, :] = wide

    row_of = lax.broadcasted_iota(jnp.int32, (56, 128), 0)
    lane_of = lax.broadcasted_iota(jnp.int32, (56, 128), 1)
    on_diag = row_of == lane_of + 28 * hi
    rs[...] = jnp.zeros_like(rs)
    rs[0:1, 0:28] = line[...]
    rs_row = rs[0:1, :]
    rx[...] = jnp.where(on_diag & (lane_of < 28), jnp.broadcast_to(rs_row, (56, 128)), 0.0)
    px[...] = jnp.where(hi == 0, pf[:, 512:1024], pf[:, 0:512]).astype(BF16)
    mate = moved("y", 2)
    push(px, pxr, xs.at[0], xr.at[0], mate, core)
    push(rx, rxr, xs.at[1], xr.at[1], mate, core)

    def add_chunk(t, a1):
        settle(w[t].at[a1], recv_k[0])
        settle(pr[t].at[a1], recv_k[1])

        def body(i, carry):
            w[t][a1, i] = w[t][a1, i] + pr[t][a1, i]
            return carry

        lax.fori_loop(0, 4, body, 0)

    for k in (2, 1, 3, 0):
        for t in range(3):
            a1 = rel(t, 0, k)
            recv_k = (recv.at[t, LD + k], recv.at[t, PR + k])
            add_chunk(t, a1)
            up, down = moved(axes[t][0], 1), moved(axes[t][0], 3)
            if k == 2:
                for n, j in enumerate((2, 1)):
                    push(w[t].at[a1, rel(t, 1, j)], rlp[t].at[n], send.at[t, 1], recv.at[t, RLP + n], up, core)
                for n, j in enumerate((3, 0)):
                    push(w[t].at[a1, rel(t, 1, j)], rlm[t].at[n], send.at[t, 1], recv.at[t, RLM + n], down, core)
            if k == 1:
                for j in (3, 0):
                    push(w[t].at[a1, rel(t, 1, j)], fm[t].at[j], send.at[t, 1], recv.at[t, FM + j], up, core)
            if k == 3:
                for j in (2, 1):
                    push(w[t].at[a1, rel(t, 1, j)], fp[t].at[j], send.at[t, 1], recv.at[t, FP + j], down, core)

    for n in range(2):
        for t in range(3):
            up, down = moved(axes[t][0], 1), moved(axes[t][0], 3)
            for k, j, buf, base, dst, dbase, to in (
                (1, (2, 1)[n], rlp[t], RLP, fm[t], FM, up),
                (3, (3, 0)[n], rlm[t], RLM, fp[t], FP, down),
            ):
                settle(buf.at[n], recv.at[t, base + n])
                a1, a2 = rel(t, 0, k), rel(t, 1, j)
                w[t][a1, a2] = w[t][a1, a2] + buf[n]
                push(w[t].at[a1, a2], dst.at[j], send.at[t, 1], recv.at[t, dbase + j], to, core)

    for j in (2, 3, 1, 0):
        for t in range(3):
            settle(fm[t].at[j], recv.at[t, FM + j])
            settle(fp[t].at[j], recv.at[t, FP + j])
            a1, a2 = rel(t, 0, 0), rel(t, 1, j)

            def body(i, carry):
                s1[t][j, i] = (w[t][a1, a2, i].astype(F32) + fm[t][j, i].astype(F32) + fp[t][j, i].astype(F32)).astype(BF16)
                return carry

            lax.fori_loop(0, 4, body, 0)
            if j:
                push(s1[t].at[j], r2[t].at[j - 1], send.at[t, 2], recv.at[t, SE + j - 1], moved(axes[t][1], j), core)

    for t in range(3):
        for j in range(3):
            settle(r2[t].at[j], recv.at[t, SE + j])
        for m in (2, 1, 3, 0):
            a3 = rel(t, 2, m)
            total = s1[t][0, a3].astype(F32)
            for j in range(3):
                total = total + r2[t][j, a3].astype(F32)
            if m:
                s2[t][m - 1] = total.astype(BF16)
                push(s2[t].at[m - 1], r3[t].at[m - 1], send.at[t, 3], recv.at[t, TH + m - 1], moved(axes[t][2], m), core)
            else:
                s3[t][...] = total
    for t in range(3):
        total = s3[t][...]
        for m in range(3):
            settle(r3[t].at[m], recv.at[t, TH + m])
            total = total + r3[t][m].astype(F32)
        s3[t][...] = total

    tiles = [s3[t][0:56, :] for t in range(3)] + [jnp.concatenate([s3[t][56 : ROWS[t], :] for t in range(3)], axis=0)]
    squares = [v * v for v in tiles]
    rq[...] = squares[0] + squares[1] + squares[2] + squares[3]
    push(rq, rqr, xs.at[2], xr.at[2], mate, core)
    sums = [jnp.sum(v, axis=0, keepdims=True) for v in squares]
    eight = jnp.concatenate(sums + sums, axis=0)
    row8 = lax.broadcasted_iota(jnp.int32, (8, 128), 0)
    eight = jnp.where((row8 >= 4 * hi) & (row8 < 4 * hi + 4), eight, 0.0)
    mine = at["x"] * 2 + core
    st1[mine, 0:8, :] = eight
    st1[mine, 8:16, :] = rs[...]
    n = 0
    for k in range(4):
        for flip in (0, 1):
            if k or flip:
                tc = core if not flip else 1 - core
                push(st1.at[mine], st1.at[mine], t1s.at[0], t1r.at[n], moved("x", k), tc)
                n += 1
    n = 0
    for k in range(4):
        for flip in (0, 1):
            if k or flip:
                settle(st1.at[0], t1r.at[n])
                n += 1
    total = st1[0]
    for i in range(1, 8):
        total = total + st1[i]
    for level, (axis, buf) in enumerate((("y", st2), ("z", st3))):
        buf[at[axis]] = total
        for k in (2, 1, 3):
            push(buf.at[at[axis]], buf.at[at[axis]], t2s.at[level], t2r.at[level, k - 1], moved(axis, k), core)
        for k in (1, 3, 2):
            settle(buf.at[0], t2r.at[level, k - 1])
        total = buf[0] + buf[1] + buf[2] + buf[3]

    column_sums = total[0:8, :]
    norm_square = jnp.sum(jnp.sum(column_sums, axis=0, keepdims=True), axis=1, keepdims=True)
    rs_total = jnp.sum(total[8:9, :], axis=1, keepdims=True)
    factor = jnp.minimum(1.0, CLIP / jnp.sqrt(norm_square + 1e-06))
    square_factor = factor * factor
    column_next = BETA * cs[...] + (1.0 - BETA) * (square_factor * column_sums * (1.0 / D))
    coln[...] = column_next
    row_average = (BETA / D) * rs_total + (1.0 - BETA) * (square_factor * norm_square * (1.0 / (D * KW)))

    for i in range(3):
        settle((pxr, rxr, rqr)[i], xr.at[i])
    row_state = jnp.sum(rx[...] + rxr[...], axis=1, keepdims=True)
    row_square = jnp.sum(rq[...] + rqr[...], axis=1, keepdims=True)
    row_next = BETA * row_state + (1.0 - BETA) * (square_factor * row_square * (1.0 / KW))
    rown_line = jnp.sum(jnp.where(on_diag, jnp.broadcast_to(row_next, (56, 128)), 0.0), axis=0, keepdims=True)
    rown[...] = rown_line[:, 0:28]

    mine_half = jnp.where(hi == 0, column_next[0:4, :], column_next[4:8, :])
    fresh = []
    for tile in range(4):
        old = jnp.where(hi == 0, pf[:, tile * 128 : tile * 128 + 128], pf[:, 512 + tile * 128 : 640 + tile * 128])
        old = old + pxr[:, tile * 128 : tile * 128 + 128].astype(F32)
        second = row_next * mine_half[tile : tile + 1, :] / row_average
        update = factor * tiles[tile] / jnp.sqrt(second)
        fresh.append((old - STEP * update).astype(BF16))
    for t in range(3):
        a1, a2, a3 = pos[t]
        own[t][a1, a2, a3, 0:56, :] = fresh[t]
        own[t][a1, a2, a3, 56 : ROWS[t], :] = fresh[3][STRIP[t][0] : STRIP[t][1], :]

    for t in range(3):
        block = own[t].at[pos[t]]
        for k in (2, 1, 3):
            push(block, block, send.at[t, 4], recv.at[t, GT + k - 1], moved(axes[t][2], k), core)

    def arrived(t, j):
        sub = own[t].at[pos[t][0], rel(t, 1, j)]
        push(sub, sub, send.at[t, 6], recv.at[t, GM + j], moved(axes[t][0], 1), core)
        push(sub, sub, send.at[t, 6], recv.at[t, GP + j], moved(axes[t][0], 3), core)
        push(sub, other[t].at[pos[t][0], rel(t, 1, j)], send.at[t, 7], recv.at[t, GC], at, 1 - core)

    for t in range(3):
        for k in (1, 3, 2):
            settle(own[t].at[0, 0, 0], recv.at[t, GT + k - 1])
        sub = own[t].at[pos[t][0], pos[t][1]]
        for k in (2, 1, 3):
            push(sub, sub, send.at[t, 5], recv.at[t, GS + k - 1], moved(axes[t][1], k), core)
        arrived(t, 0)
    for j in (1, 3, 2):
        for t in range(3):
            settle(own[t].at[0, 0], recv.at[t, GS + (4 - j) - 1])
            arrived(t, j)

    for j in (0, 1, 3, 2):
        for t in range(3):
            for base, k, onward in ((GM, 3, 1), (GP, 1, 3)):
                sub = own[t].at[rel(t, 0, k), rel(t, 1, j)]
                settle(sub, recv.at[t, base + j])
                if (j in (0, 3)) == (onward == 1):
                    push(sub, sub, send.at[t, 6], recv.at[t, GO + j], moved(axes[t][0], onward), core)
                push(sub, other[t].at[rel(t, 0, k), rel(t, 1, j)], send.at[t, 7], recv.at[t, GC], at, 1 - core)
    for j in (0, 1, 3, 2):
        for t in range(3):
            sub = own[t].at[rel(t, 0, 2), rel(t, 1, j)]
            settle(sub, recv.at[t, GO + j])
            push(sub, other[t].at[rel(t, 0, 2), rel(t, 1, j)], send.at[t, 7], recv.at[t, GC], at, 1 - core)

    for h in (0, 1):
        here = dict(at, y=2 * h + lo)
        blocks = [own[t].at[tuple(here[a] for a in axes[t])] for t in range(3)]
        for t in range(3):
            pf[:, 512 * h + 128 * t : 512 * h + 128 * t + 128] = blocks[t][0:56, :].astype(F32)
            pf[STRIP[t][0] : STRIP[t][1], 512 * h + 384 : 512 * h + 512] = blocks[t][56 : ROWS[t], :].astype(F32)
    newp[...] = jnp.where(hi == 0, pf[0:28, :], pf[28:56, :]).astype(BF16)

    for t in range(3):
        settle(w[t], send.at[t, 0])
        settle(w[t].at[0:3], send.at[t, 1])
        settle(w[t].at[0, 0:3], send.at[t, 2])
        settle(w[t].at[0, 0, 0:3], send.at[t, 3])
        settle(w[t].at[0, 0, 0:3], send.at[t, 4])
        settle(w[t].at[0, 0:3], send.at[t, 5])
        settle(w[t].at[0:3], send.at[t, 6])
        settle(w[t], send.at[t, 7])
        settle(other[t], recv.at[t, GC])
    for i in range(3):
        settle((px, rx, rq)[i], xs.at[i])
    settle(st1.at[0:7], t1s.at[0])
    for level, buf in enumerate((st2, st3)):
        settle(buf.at[0:3], t2s.at[level])


def layout_kernel(*refs):
    own, other = refs[0:3], refs[3:6]
    newp, rown, coln = refs[6:9]
    whole, newp_out, rown_out, coln_out, sems = refs[9:]
    _, _, _, core = where_am_i()
    for src, dst in ((newp, newp_out), (rown, rown_out), (coln, coln_out)):
        pltpu.make_async_copy(src, dst, sems.at[3]).start()
    for held, c in ((own, core), (other, 1 - core)):
        for t in range(3):
            for a1 in range(4):
                for dst, src in copies(t, a1, c, whole, held[t]):
                    pltpu.make_async_copy(src, dst, sems.at[t]).start()
    for t in range(3):
        for held in (own, other):
            pltpu.make_async_copy(held[t], held[t], sems.at[t]).wait()
    for src, dst in ((newp, newp_out), (rown, rown_out), (coln, coln_out)):
        pltpu.make_async_copy(src, dst, sems.at[3]).wait()


def solution(mesh):
    block = [(r, 128) for r in ROWS]
    part = [jax.ShapeDtypeStruct((4, 4, 4) + b, BF16) for b in block]
    vmem = pl.BlockSpec(memory_space=pltpu.VMEM)
    anywhere = pl.BlockSpec(memory_space=pl.ANY)

    def local(grad_bucket, parameters, row_state, column_state):
        def three(*lead, dtype=BF16):
            return [pltpu.VMEM(lead + b, dtype) for b in block]

        scratch = (
            three(4, 4, 4) + three(4, 4, 4) + three(2, 4) + three(2, 4) + three(4, 4) + three(4, 4) + three(4, 4)
            + three(3, 4) + three(3) + three(3) + three(dtype=F32)
            + [
                pltpu.VMEM((28, KW), BF16), pltpu.VMEM((1, 28), F32), pltpu.VMEM((8, 128), F32), pltpu.VMEM((8, 128), F32),
                pltpu.VMEM((56, 1024), F32),
                pltpu.VMEM((56, 512), BF16), pltpu.VMEM((56, 512), BF16),
                pltpu.VMEM((56, 128), F32), pltpu.VMEM((56, 128), F32),
                pltpu.VMEM((56, 128), F32), pltpu.VMEM((56, 128), F32),
                pltpu.VMEM((8, 16, 128), F32), pltpu.VMEM((4, 16, 128), F32), pltpu.VMEM((4, 16, 128), F32),
                pltpu.SemaphoreType.DMA((3, NRECV)), pltpu.SemaphoreType.DMA((3, NSEND)),
                pltpu.SemaphoreType.DMA((3,)), pltpu.SemaphoreType.DMA((3,)),
                pltpu.SemaphoreType.DMA((7,)), pltpu.SemaphoreType.DMA((1,)),
                pltpu.SemaphoreType.DMA((2, 3)), pltpu.SemaphoreType.DMA((2,)),
                pltpu.SemaphoreType.DMA((3,)),
            ]
        )
        small = [
            jax.ShapeDtypeStruct((28, KW), BF16),
            jax.ShapeDtypeStruct((1, 28), F32),
            jax.ShapeDtypeStruct((8, 128), F32),
        ]
        held = pl.pallas_call(
            step_kernel,
            out_shape=part + part + small,
            in_specs=[pl.BlockSpec(memory_space=pltpu.HBM)] * 4,
            out_specs=[vmem] * 9,
            scratch_shapes=scratch,
            compiler_params=pltpu.CompilerParams(
                collective_id=0, has_side_effects=True, vmem_limit_bytes=40 * 1024 * 1024
            ),
            name="adafactor_step",
        )(
            grad_bucket.reshape(4, 2, 2, 4, 56, KW),
            parameters.reshape(28, KW),
            row_state,
            column_state.reshape(8, 128),
        )
        whole, newp, rown, coln = pl.pallas_call(
            layout_kernel,
            out_shape=[jax.ShapeDtypeStruct((4, 2, 2, 4, 56, KW), BF16)] + small,
            in_specs=[vmem] * 9,
            out_specs=[anywhere] * 4,
            scratch_shapes=[pltpu.SemaphoreType.DMA((4,))],
            compiler_params=pltpu.CompilerParams(vmem_limit_bytes=20 * 1024 * 1024),
            name="lay_out",
        )(*held)
        return newp.reshape(1, 28, KW), rown, coln.reshape(1, KW), whole.reshape(D, KW)

    every = ("gx", "gy", "gz")
    return jax.shard_map(
        local,
        mesh=mesh,
        in_specs=(P(every, None, None, None), P(None, every, None), P(None, every), P(None, None)),
        out_specs=(P(None, every, None), P(None, every), P(None, None), P(None, None)),
        check_vma=False,
    )
```

```python
import math

import jax
import jax.numpy as jnp
from jax import lax
from jax.experimental import pallas as pl
from jax.experimental.pallas import tpu as pltpu
from jax.sharding import PartitionSpec as P

D = 3584
KW = 1024
CLIP = 0.5 * math.sqrt(D * KW)
BETA = 0.8
STEP = 0.5
MESH = pl.DeviceIdType.MESH
F32 = jnp.float32
BF16 = jnp.bfloat16

ORDER = ("xyz", "yzx", "zxy")
STRIP = ((0, 24), (24, 40), (40, 56))
ROWS = tuple(56 + b - a for a, b in STRIP)
LD, PR, RLP, RLM, FM, FP, SE, TH = 0, 4, 8, 12, 16, 20, 24, 36
GT, GS, GM, GP, GO, GC = 39, 42, 45, 49, 53, 57
NRECV = 58
NSEND = 8


def mod4(v):
    return lax.rem(v, 4)


def where_am_i():
    gx, gy, gz = lax.axis_index("gx"), lax.axis_index("gy"), lax.axis_index("gz")
    lo, core = lax.div(gy, 2), lax.rem(gy, 2)
    z, hi = lax.div(gz, 2), lax.rem(gz, 2)
    return {"x": gx, "y": 2 * hi + lo, "z": z}, lo, hi, core


def device(at, core):
    return (at["x"], lax.rem(at["y"], 2) * 2 + core, at["z"] * 2 + lax.div(at["y"], 2))


def pieces(t, a1):
    every = slice(None)
    if t == 0:
        return [((a1, every, None, every), h, (pl.ds(2 * h, 2), every)) for h in (0, 1)]
    if t == 1:
        hi, lo = lax.div(a1, 2), lax.rem(a1, 2)
        return [((every, lo, None, z), hi, (z, every)) for z in range(4)]
    return [((every, every, None, a1), h, (every, pl.ds(2 * h, 2))) for h in (0, 1)]


def rectangles(t):
    return [(t, 0, 56, 0), (3, STRIP[t][0], STRIP[t][1], 56)]


def copies(t, a1, core, whole, part):
    out = []
    for (x, lo, _, z), h, (i, j) in pieces(t, a1):
        for tile, r0, r1, d0 in rectangles(t):
            col = h * 512 + tile * 128
            if not isinstance(col, int):
                col = pl.multiple_of(col, 128)
            out.append((
                whole.at[x, lo, core, z, pl.ds(r0, r1 - r0), pl.ds(col, 128)],
                part.at[a1, i, j, pl.ds(d0, r1 - r0), :],
            ))
    return out


def step_kernel(*refs):
    (g, par_in, rs_in, cs_in), refs = refs[:4], refs[4:]
    outs, refs = refs[:9], refs[9:]
    own, other = outs[0:3], outs[3:6]
    newp, rown, coln = outs[6:9]
    it = iter(refs)
    take3 = lambda: [next(it) for _ in range(3)]
    w, pr, rlp, rlm, fm, fp, s1, r2, s2, r3, s3 = (take3() for _ in range(11))
    par, line, rs, cs, pf, px, pxr, rx, rxr, rq, rqr, st1, st2 = (next(it) for _ in range(13))
    recv, send, xr, xs, t1r, t1s, t2r, t2s, near = (next(it) for _ in range(9))

    at, lo, hi, core = where_am_i()

    def moved(axis, k):
        to = dict(at)
        to[axis] = mod4(at[axis] + k)
        return to

    def push(src, dst, ssem, rsem, to, tc):
        pltpu.make_async_remote_copy(
            src_ref=src, dst_ref=dst, send_sem=ssem, recv_sem=rsem, device_id=device(to, tc), device_id_type=MESH
        ).start()

    def settle(ref, sem):
        pltpu.make_async_copy(ref, ref, sem).wait()

    axes = [tuple(ORDER[t]) for t in range(3)]
    pos = [tuple(at[a] for a in axes[t]) for t in range(3)]

    def rel(t, level, k):
        return mod4(pos[t][level] + k)

    small = ((par_in, par), (rs_in, line), (cs_in, cs))
    for i, (src, dst) in enumerate(small):
        pltpu.make_async_copy(src, dst, near.at[i]).start()
    for k in (2, 1, 3, 0):
        for t in range(3):
            for src, dst in copies(t, rel(t, 0, k), core, g, w[t]):
                pltpu.make_async_copy(src, dst, recv.at[t, LD + k]).start()

    barrier = pltpu.get_barrier_semaphore()
    for axis in "xyz":
        for k in (1, 3):
            pl.semaphore_signal(barrier, inc=1, device_id=device(moved(axis, k), core), device_id_type=MESH)
    pl.semaphore_signal(barrier, inc=1, device_id=device(at, 1 - core), device_id_type=MESH)
    pl.semaphore_wait(barrier, 7)

    for k in (2, 1, 3, 0):
        for t in range(3):
            for src, (_, dst) in zip(
                [s for s, _ in copies(t, rel(t, 0, k), 1 - core, g, pr[t])], copies(t, rel(t, 0, k), core, g, pr[t])
            ):
                push(src, dst, send.at[t, 0], recv.at[t, PR + k], at, 1 - core)

    pf[...] = jnp.zeros_like(pf)
    for i, (src, dst) in enumerate(small):
        pltpu.make_async_copy(src, dst, near.at[i]).wait()
    wide = par[...].astype(F32)

    @pl.when(hi == 0)
    def _():
        pf[0:28, :] = wide

    @pl.when(hi == 1)
    def _():
        pf[28:56, :] = wide

    row_of = lax.broadcasted_iota(jnp.int32, (56, 128), 0)
    lane_of = lax.broadcasted_iota(jnp.int32, (56, 128), 1)
    on_diag = row_of == lane_of + 28 * hi
    rs[...] = jnp.zeros_like(rs)
    rs[0:1, 0:28] = line[...]
    rs_row = rs[0:1, :]
    rx[...] = jnp.where(on_diag & (lane_of < 28), jnp.broadcast_to(rs_row, (56, 128)), 0.0)
    px[...] = jnp.where(hi == 0, pf[:, 512:1024], pf[:, 0:512]).astype(BF16)
    mate = moved("y", 2)

    def add_chunk(t, a1):
        settle(w[t].at[a1], recv_k[0])
        settle(pr[t].at[a1], recv_k[1])

        def body(i, carry):
            w[t][a1, i] = w[t][a1, i] + pr[t][a1, i]
            return carry

        lax.fori_loop(0, 4, body, 0)

    for k in (2, 1, 3, 0):
        for t in range(3):
            a1 = rel(t, 0, k)
            recv_k = (recv.at[t, LD + k], recv.at[t, PR + k])
            add_chunk(t, a1)
            up, down = moved(axes[t][0], 1), moved(axes[t][0], 3)
            if k == 2:
                for j in (2, 3, 1, 0):
                    sub = w[t].at[a1, rel(t, 1, j)]
                    push(sub.at[0:2], rlp[t].at[j], send.at[t, 1], recv.at[t, RLP + j], up, core)
                    push(sub.at[2:4], rlm[t].at[j], send.at[t, 1], recv.at[t, RLM + j], down, core)
            if k == 1:
                for j in (2, 3, 1, 0):
                    sub = w[t].at[a1, rel(t, 1, j)]
                    push(sub.at[2:4], fm[t].at[j, 2:4], send.at[t, 1], recv.at[t, FM + j], up, core)
            if k == 3:
                for j in (2, 3, 1, 0):
                    sub = w[t].at[a1, rel(t, 1, j)]
                    push(sub.at[0:2], fp[t].at[j, 0:2], send.at[t, 1], recv.at[t, FP + j], down, core)

    for j in (2, 3, 1, 0):
        for t in range(3):
            up, down = moved(axes[t][0], 1), moved(axes[t][0], 3)
            for k, half, buf, base, dst, dbase, to in (
                (1, 0, rlp[t], RLP, fm[t], FM, up),
                (3, 2, rlm[t], RLM, fp[t], FP, down),
            ):
                settle(buf.at[j], recv.at[t, base + j])
                a1, a2 = rel(t, 0, k), rel(t, 1, j)
                w[t][a1, a2, half : half + 2] = w[t][a1, a2, half : half + 2] + buf[j]
                push(
                    w[t].at[a1, a2, half : half + 2], dst.at[j, half : half + 2],
                    send.at[t, 1], recv.at[t, dbase + j], to, core,
                )
    push(px, pxr, xs.at[0], xr.at[0], mate, core)
    push(rx, rxr, xs.at[1], xr.at[1], mate, core)

    for j in (2, 3, 1, 0):
        for t in range(3):
            settle(fm[t].at[j], recv.at[t, FM + j])
            settle(fp[t].at[j], recv.at[t, FP + j])
            a1, a2 = rel(t, 0, 0), rel(t, 1, j)
            for m in (2, 1, 3, 0):
                a3 = rel(t, 2, m)
                s1[t][j, a3] = (
                    w[t][a1, a2, a3].astype(F32) + fm[t][j, a3].astype(F32) + fp[t][j, a3].astype(F32)
                ).astype(BF16)
                if j:
                    push(
                        s1[t].at[j, a3], r2[t].at[j - 1, a3],
                        send.at[t, 2], recv.at[t, SE + 4 * (j - 1) + m], moved(axes[t][1], j), core,
                    )

    for m in (2, 1, 3, 0):
        for t in range(3):
            a3 = rel(t, 2, m)
            total = s1[t][0, a3].astype(F32)
            for j in (1, 2, 0):
                settle(r2[t].at[j, a3], recv.at[t, SE + 4 * j + m])
                total = total + r2[t][j, a3].astype(F32)
            if m:
                s2[t][m - 1] = total.astype(BF16)
                push(s2[t].at[m - 1], r3[t].at[m - 1], send.at[t, 3], recv.at[t, TH + m - 1], moved(axes[t][2], m), core)
            else:
                s3[t][...] = total
    for t in range(3):
        total = s3[t][...]
        for m in (0, 2, 1):
            settle(r3[t].at[m], recv.at[t, TH + m])
            total = total + r3[t][m].astype(F32)
        s3[t][...] = total

    tiles = [s3[t][0:56, :] for t in range(3)] + [jnp.concatenate([s3[t][56 : ROWS[t], :] for t in range(3)], axis=0)]
    squares = [v * v for v in tiles]
    rq[...] = squares[0] + squares[1] + squares[2] + squares[3]
    push(rq, rqr, xs.at[2], xr.at[2], mate, core)
    sums = [jnp.sum(v, axis=0, keepdims=True) for v in squares]
    mine = at["x"] * 2 + core
    st1[mine] = jnp.concatenate(sums + [rs_row, jnp.zeros((3, 128), F32)], axis=0)
    near_group = [(k, flip) for k in (2, 1, 3, 0) for flip in (1, 0) if k or flip]
    for n, (k, flip) in enumerate(near_group):
        push(st1.at[mine], st1.at[mine], t1s.at[0], t1r.at[n], moved("x", k), 1 - core if flip else core)

    def added(buf, lo_slot, hi_slot):
        terms = [buf[i] for i in range(lo_slot, hi_slot)]
        while len(terms) > 1:
            terms = [a + b for a, b in zip(terms[0::2], terms[1::2])]
        return terms[0]

    olds = []
    for i in range(2):
        settle((pxr, rxr)[i], xr.at[i])
    for tile in range(4):
        old = jnp.where(hi == 0, pf[:, tile * 128 : tile * 128 + 128], pf[:, 512 + tile * 128 : 640 + tile * 128])
        olds.append(old + pxr[:, tile * 128 : tile * 128 + 128].astype(F32))
    row_state = jnp.sum(rx[...] + rxr[...], axis=1, keepdims=True)

    for n in range(7):
        settle(st1.at[0], t1r.at[n])
    slot = at["y"] * 4 + at["z"]
    st2[slot] = added(st1, 0, 8)
    far_group = [(i, j) for i in (2, 1, 3, 0) for j in (2, 1, 3, 0) if i or j]
    for n, (i, j) in enumerate(far_group):
        to = dict(moved("y", i), z=mod4(at["z"] + j))
        push(st2.at[slot], st2.at[slot], t2s.at[0], t2r.at[n], to, core)
    settle(rqr, xr.at[2])
    row_square = jnp.sum(rq[...] + rqr[...], axis=1, keepdims=True)
    for n in range(15):
        settle(st2.at[0], t2r.at[n])
    half0, half1 = added(st2, 0, 8), added(st2, 8, 16)

    column_sums = jnp.concatenate([half0[0:4, :], half1[0:4, :]], axis=0)
    norm_square = jnp.sum(jnp.sum(column_sums, axis=0, keepdims=True), axis=1, keepdims=True)
    rs_total = jnp.sum(half0[4:5, :] + half1[4:5, :], axis=1, keepdims=True)
    factor = jnp.minimum(1.0, CLIP / jnp.sqrt(norm_square + 1e-06))
    square_factor = factor * factor
    column_next = BETA * cs[...] + (1.0 - BETA) * (square_factor * column_sums * (1.0 / D))
    row_average = (BETA / D) * rs_total + (1.0 - BETA) * (square_factor * norm_square * (1.0 / (D * KW)))
    row_next = BETA * row_state + (1.0 - BETA) * (square_factor * row_square * (1.0 / KW))

    mine_half = jnp.where(hi == 0, column_next[0:4, :], column_next[4:8, :])
    fresh = []
    for tile in range(4):
        second = row_next * mine_half[tile : tile + 1, :] / row_average
        update = factor * tiles[tile] / jnp.sqrt(second)
        fresh.append((olds[tile] - STEP * update).astype(BF16))
    for t in range(3):
        a1, a2, a3 = pos[t]
        own[t][a1, a2, a3, 0:56, :] = fresh[t]
        own[t][a1, a2, a3, 56 : ROWS[t], :] = fresh[3][STRIP[t][0] : STRIP[t][1], :]

    for t in range(3):
        block = own[t].at[pos[t]]
        for k in (2, 1, 3):
            push(block, block, send.at[t, 4], recv.at[t, GT + k - 1], moved(axes[t][2], k), core)

    def onward(t, block, j):
        push(block, block, send.at[t, 6], recv.at[t, GM + j], moved(axes[t][0], 1), core)
        push(block, block, send.at[t, 6], recv.at[t, GP + j], moved(axes[t][0], 3), core)

    def across(t, a1, a2):
        push(own[t].at[a1, a2], other[t].at[a1, a2], send.at[t, 7], recv.at[t, GC], at, 1 - core)

    for m in (0, 1, 3, 2):
        for t in range(3):
            block = own[t].at[pos[t][0], pos[t][1], rel(t, 2, m)]
            if m:
                settle(block, recv.at[t, GT + (4 - m) - 1])
            for k in (2, 1, 3):
                push(block, block, send.at[t, 5], recv.at[t, GS + k - 1], moved(axes[t][1], k), core)
            onward(t, block, 0)
    for t in range(3):
        across(t, pos[t][0], pos[t][1])
    for j in (1, 3, 2):
        for t in range(3):
            sub = own[t].at[pos[t][0], rel(t, 1, j)]
            settle(sub, recv.at[t, GS + (4 - j) - 1])
            onward(t, sub, j)
            across(t, pos[t][0], rel(t, 1, j))

    for j in (0, 1, 3, 2):
        for t in range(3):
            for base, k, shift in ((GM, 3, 1), (GP, 1, 3)):
                sub = own[t].at[rel(t, 0, k), rel(t, 1, j)]
                settle(sub, recv.at[t, base + j])
                if (j in (0, 3)) == (shift == 1):
                    push(sub, sub, send.at[t, 6], recv.at[t, GO + j], moved(axes[t][0], shift), core)
                across(t, rel(t, 0, k), rel(t, 1, j))
    coln[...] = column_next
    rown_line = jnp.sum(jnp.where(on_diag, jnp.broadcast_to(row_next, (56, 128)), 0.0), axis=0, keepdims=True)
    rown[...] = rown_line[:, 0:28]
    for j in (0, 1, 3, 2):
        for t in range(3):
            settle(own[t].at[rel(t, 0, 2), rel(t, 1, j)], recv.at[t, GO + j])
            across(t, rel(t, 0, 2), rel(t, 1, j))

    for h in (0, 1):
        here = dict(at, y=2 * h + lo)
        blocks = [own[t].at[tuple(here[a] for a in axes[t])] for t in range(3)]
        for t in range(3):
            pf[:, 512 * h + 128 * t : 512 * h + 128 * t + 128] = blocks[t][0:56, :].astype(F32)
            pf[STRIP[t][0] : STRIP[t][1], 512 * h + 384 : 512 * h + 512] = blocks[t][56 : ROWS[t], :].astype(F32)
    newp[...] = jnp.where(hi == 0, pf[0:28, :], pf[28:56, :]).astype(BF16)

    for t in range(3):
        settle(w[t], send.at[t, 0])
        settle(w[t].at[0:3], send.at[t, 1])
        settle(w[t].at[0, 0:3], send.at[t, 2])
        settle(w[t].at[0, 0, 0:3], send.at[t, 3])
        settle(w[t].at[0, 0, 0:3], send.at[t, 4])
        settle(w[t].at[0, 0:3], send.at[t, 5])
        settle(w[t].at[0:3], send.at[t, 6])
        settle(w[t], send.at[t, 7])
        settle(other[t], recv.at[t, GC])
    for i in range(3):
        settle((px, rx, rq)[i], xs.at[i])
    settle(st1.at[0:7], t1s.at[0])
    settle(st2.at[0:15], t2s.at[0])


def layout_kernel(*refs):
    own, other = refs[0:3], refs[3:6]
    newp, rown, coln = refs[6:9]
    whole, newp_out, rown_out, coln_out, sems = refs[9:]
    _, _, _, core = where_am_i()
    for src, dst in ((newp, newp_out), (rown, rown_out), (coln, coln_out)):
        pltpu.make_async_copy(src, dst, sems.at[3]).start()
    for held, c in ((own, core), (other, 1 - core)):
        for t in range(3):
            for a1 in range(4):
                for dst, src in copies(t, a1, c, whole, held[t]):
                    pltpu.make_async_copy(src, dst, sems.at[t]).start()
    for t in range(3):
        for held in (own, other):
            pltpu.make_async_copy(held[t], held[t], sems.at[t]).wait()
    for src, dst in ((newp, newp_out), (rown, rown_out), (coln, coln_out)):
        pltpu.make_async_copy(src, dst, sems.at[3]).wait()


def solution(mesh):
    block = [(r, 128) for r in ROWS]
    part = [jax.ShapeDtypeStruct((4, 4, 4) + b, BF16) for b in block]
    vmem = pl.BlockSpec(memory_space=pltpu.VMEM)
    anywhere = pl.BlockSpec(memory_space=pl.ANY)

    def hbm(v):
        return pltpu.with_memory_space_constraint(v, pltpu.HBM)

    def local(grad_bucket, parameters, row_state, column_state):
        def three(*lead, dtype=BF16):
            return [pltpu.VMEM(lead + b, dtype) for b in block]

        scratch = (
            three(4, 4, 4) + three(4, 4, 4) + three(4, 2) + three(4, 2) + three(4, 4) + three(4, 4) + three(4, 4)
            + three(3, 4) + three(3) + three(3) + three(dtype=F32)
            + [
                pltpu.VMEM((28, KW), BF16), pltpu.VMEM((1, 28), F32), pltpu.VMEM((8, 128), F32), pltpu.VMEM((8, 128), F32),
                pltpu.VMEM((56, 1024), F32),
                pltpu.VMEM((56, 512), BF16), pltpu.VMEM((56, 512), BF16),
                pltpu.VMEM((56, 128), F32), pltpu.VMEM((56, 128), F32),
                pltpu.VMEM((56, 128), F32), pltpu.VMEM((56, 128), F32),
                pltpu.VMEM((8, 8, 128), F32), pltpu.VMEM((16, 8, 128), F32),
                pltpu.SemaphoreType.DMA((3, NRECV)), pltpu.SemaphoreType.DMA((3, NSEND)),
                pltpu.SemaphoreType.DMA((3,)), pltpu.SemaphoreType.DMA((3,)),
                pltpu.SemaphoreType.DMA((7,)), pltpu.SemaphoreType.DMA((1,)),
                pltpu.SemaphoreType.DMA((15,)), pltpu.SemaphoreType.DMA((1,)),
                pltpu.SemaphoreType.DMA((3,)),
            ]
        )
        small = [
            jax.ShapeDtypeStruct((28, KW), BF16),
            jax.ShapeDtypeStruct((1, 28), F32),
            jax.ShapeDtypeStruct((8, 128), F32),
        ]
        held = pl.pallas_call(
            step_kernel,
            out_shape=part + part + small,
            in_specs=[pl.BlockSpec(memory_space=pltpu.HBM)] * 4,
            out_specs=[vmem] * 9,
            scratch_shapes=scratch,
            compiler_params=pltpu.CompilerParams(
                collective_id=0, has_side_effects=True, vmem_limit_bytes=40 * 1024 * 1024
            ),
            name="adafactor_step",
        )(
            grad_bucket.reshape(4, 2, 2, 4, 56, KW),
            hbm(parameters.reshape(28, KW)),
            hbm(row_state),
            hbm(column_state.reshape(8, 128)),
        )
        whole, newp, rown, coln = pl.pallas_call(
            layout_kernel,
            out_shape=[jax.ShapeDtypeStruct((4, 2, 2, 4, 56, KW), BF16)] + small,
            in_specs=[vmem] * 9,
            out_specs=[anywhere] * 4,
            scratch_shapes=[pltpu.SemaphoreType.DMA((4,))],
            compiler_params=pltpu.CompilerParams(vmem_limit_bytes=20 * 1024 * 1024),
            name="lay_out",
        )(*held)
        return newp.reshape(1, 28, KW), rown, coln.reshape(1, KW), whole.reshape(D, KW)

    every = ("gx", "gy", "gz")
    return jax.shard_map(
        local,
        mesh=mesh,
        in_specs=(P(every, None, None, None), P(None, every, None), P(None, every), P(None, None)),
        out_specs=(P(None, every, None), P(None, every), P(None, None), P(None, None)),
        check_vma=False,
    )
```

```python
import math

import jax
import jax.numpy as jnp
from jax import lax
from jax.experimental import pallas as pl
from jax.experimental.pallas import tpu as pltpu
from jax.sharding import PartitionSpec as P

D = 3584
KW = 1024
CLIP = 0.5 * math.sqrt(D * KW)
BETA = 0.8
STEP = 0.5
MESH = pl.DeviceIdType.MESH
F32 = jnp.float32
BF16 = jnp.bfloat16

ORDER = ("xyz", "yzx", "zxy")
STRIP = ((0, 24), (24, 40), (40, 56))
ROWS = tuple(56 + b - a for a, b in STRIP)
LD, PR, RLP, RLM, FM, FP, SE, TH = 0, 4, 8, 12, 16, 20, 24, 36
GT, GS, GM, GP, GO, GC, PT, PS = 39, 42, 45, 49, 53, 57, 58, 61
NRECV = 64
NSEND = 10


def mod4(v):
    return lax.rem(v, 4)


def where_am_i():
    gx, gy, gz = lax.axis_index("gx"), lax.axis_index("gy"), lax.axis_index("gz")
    lo, core = lax.div(gy, 2), lax.rem(gy, 2)
    z, hi = lax.div(gz, 2), lax.rem(gz, 2)
    return {"x": gx, "y": 2 * hi + lo, "z": z}, lo, hi, core


def device(at, core):
    return (at["x"], lax.rem(at["y"], 2) * 2 + core, at["z"] * 2 + lax.div(at["y"], 2))


def pieces(t, a1):
    every = slice(None)
    if t == 0:
        return [((a1, every, None, every), h, (pl.ds(2 * h, 2), every)) for h in (0, 1)]
    if t == 1:
        hi, lo = lax.div(a1, 2), lax.rem(a1, 2)
        return [((every, lo, None, z), hi, (z, every)) for z in range(4)]
    return [((every, every, None, a1), h, (every, pl.ds(2 * h, 2))) for h in (0, 1)]


def rectangles(t):
    return [(t, 0, 56, 0), (3, STRIP[t][0], STRIP[t][1], 56)]


def copies(t, a1, core, whole, part):
    out = []
    for (x, lo, _, z), h, (i, j) in pieces(t, a1):
        for tile, r0, r1, d0 in rectangles(t):
            col = h * 512 + tile * 128
            if not isinstance(col, int):
                col = pl.multiple_of(col, 128)
            out.append((
                whole.at[x, lo, core, z, pl.ds(r0, r1 - r0), pl.ds(col, 128)],
                part.at[a1, i, j, pl.ds(d0, r1 - r0), :],
            ))
    return out


def step_kernel(*refs):
    (g, par_in, rs_in, cs_in), refs = refs[:4], refs[4:]
    outs, refs = refs[:9], refs[9:]
    own, other = outs[0:3], outs[3:6]
    newp, rown, coln = outs[6:9]
    it = iter(refs)
    take3 = lambda: [next(it) for _ in range(3)]
    w, pr, rlp, rlm, fm, fp, s1, r2, s2, r3, s3, sg, pg = (take3() for _ in range(13))
    par, line, rs, cs, pf, px, pxr, st1, st2, rb, rn, rf, cf = (next(it) for _ in range(13))
    recv, send, xr, xs, t1r, t1s, t2r, t2s, t3r, t3s, near = (next(it) for _ in range(11))

    at, lo, hi, core = where_am_i()

    def moved(axis, k):
        to = dict(at)
        to[axis] = mod4(at[axis] + k)
        return to

    def push(src, dst, ssem, rsem, to, tc):
        pltpu.make_async_remote_copy(
            src_ref=src, dst_ref=dst, send_sem=ssem, recv_sem=rsem, device_id=device(to, tc), device_id_type=MESH
        ).start()

    def settle(ref, sem):
        pltpu.make_async_copy(ref, ref, sem).wait()

    axes = [tuple(ORDER[t]) for t in range(3)]
    pos = [tuple(at[a] for a in axes[t]) for t in range(3)]

    def rel(t, level, k):
        return mod4(pos[t][level] + k)

    small = ((par_in, par), (rs_in, line), (cs_in, cs))
    for i, (src, dst) in enumerate(small):
        pltpu.make_async_copy(src, dst, near.at[i]).start()
    for k in (2, 1, 3, 0):
        for t in range(3):
            for src, dst in copies(t, rel(t, 0, k), core, g, w[t]):
                pltpu.make_async_copy(src, dst, recv.at[t, LD + k]).start()

    barrier = pltpu.get_barrier_semaphore()
    for axis in "xyz":
        for k in (1, 3):
            pl.semaphore_signal(barrier, inc=1, device_id=device(moved(axis, k), core), device_id_type=MESH)
    pl.semaphore_signal(barrier, inc=1, device_id=device(moved("y", 2), core), device_id_type=MESH)
    pl.semaphore_signal(barrier, inc=1, device_id=device(at, 1 - core), device_id_type=MESH)
    pl.semaphore_wait(barrier, 8)

    for k in (2, 1, 3, 0):
        for t in range(3):
            for src, (_, dst) in zip(
                [s for s, _ in copies(t, rel(t, 0, k), 1 - core, g, pr[t])], copies(t, rel(t, 0, k), core, g, pr[t])
            ):
                push(src, dst, send.at[t, 0], recv.at[t, PR + k], at, 1 - core)

    pf[...] = jnp.zeros_like(pf)
    for i, (src, dst) in enumerate(small):
        pltpu.make_async_copy(src, dst, near.at[i]).wait()
    wide = par[...].astype(F32)

    @pl.when(hi == 0)
    def _():
        pf[0:28, :] = wide

    @pl.when(hi == 1)
    def _():
        pf[28:56, :] = wide

    row_of = lax.broadcasted_iota(jnp.int32, (56, 128), 0)
    lane_of = lax.broadcasted_iota(jnp.int32, (56, 128), 1)
    on_diag = row_of == lane_of + 28 * hi
    rs[...] = jnp.zeros_like(rs)
    rs[0:1, 0:28] = line[...]
    rs_row = rs[0:1, :]
    rs_column = jnp.sum(jnp.where(on_diag & (lane_of < 28), jnp.broadcast_to(rs_row, (56, 128)), 0.0), axis=1, keepdims=True)

    def as_row(column):
        return jnp.sum(jnp.where(row_of == lane_of, jnp.broadcast_to(column, (56, 128)), 0.0), axis=0, keepdims=True)

    def as_column(row):
        return jnp.sum(jnp.where(row_of == lane_of, jnp.broadcast_to(row, (56, 128)), 0.0), axis=1, keepdims=True)

    rs_row = as_row(rs_column)
    px[...] = jnp.where(hi == 0, pf[:, 512:1024], pf[:, 0:512]).astype(BF16)
    push(px, pxr, xs.at[0], xr.at[0], moved("y", 2), core)

    def add_chunk(t, a1):
        settle(w[t].at[a1], recv_k[0])
        settle(pr[t].at[a1], recv_k[1])

        def body(i, carry):
            w[t][a1, i] = w[t][a1, i] + pr[t][a1, i]
            return carry

        lax.fori_loop(0, 4, body, 0)

    for k in (2, 1, 3, 0):
        for t in range(3):
            a1 = rel(t, 0, k)
            recv_k = (recv.at[t, LD + k], recv.at[t, PR + k])
            add_chunk(t, a1)
            up, down = moved(axes[t][0], 1), moved(axes[t][0], 3)
            if k == 2:
                for j in (2, 3, 1, 0):
                    sub = w[t].at[a1, rel(t, 1, j)]
                    push(sub.at[0:2], rlp[t].at[j], send.at[t, 1], recv.at[t, RLP + j], up, core)
                    push(sub.at[2:4], rlm[t].at[j], send.at[t, 1], recv.at[t, RLM + j], down, core)
            if k == 1:
                for j in (2, 3, 1, 0):
                    sub = w[t].at[a1, rel(t, 1, j)]
                    push(sub.at[2:4], fm[t].at[j, 2:4], send.at[t, 1], recv.at[t, FM + j], up, core)
            if k == 3:
                for j in (2, 3, 1, 0):
                    sub = w[t].at[a1, rel(t, 1, j)]
                    push(sub.at[0:2], fp[t].at[j, 0:2], send.at[t, 1], recv.at[t, FP + j], down, core)

    for j in (2, 3, 1, 0):
        for t in range(3):
            up, down = moved(axes[t][0], 1), moved(axes[t][0], 3)
            for k, half, buf, base, dst, dbase, to in (
                (1, 0, rlp[t], RLP, fm[t], FM, up),
                (3, 2, rlm[t], RLM, fp[t], FP, down),
            ):
                settle(buf.at[j], recv.at[t, base + j])
                a1, a2 = rel(t, 0, k), rel(t, 1, j)
                w[t][a1, a2, half : half + 2] = w[t][a1, a2, half : half + 2] + buf[j]
                push(
                    w[t].at[a1, a2, half : half + 2], dst.at[j, half : half + 2],
                    send.at[t, 1], recv.at[t, dbase + j], to, core,
                )

    for j in (2, 3, 1, 0):
        for t in range(3):
            settle(fm[t].at[j], recv.at[t, FM + j])
            settle(fp[t].at[j], recv.at[t, FP + j])
            a1, a2 = rel(t, 0, 0), rel(t, 1, j)
            for m in (2, 1, 3, 0):
                a3 = rel(t, 2, m)
                s1[t][j, a3] = (
                    w[t][a1, a2, a3].astype(F32) + fm[t][j, a3].astype(F32) + fp[t][j, a3].astype(F32)
                ).astype(BF16)
                if j:
                    push(
                        s1[t].at[j, a3], r2[t].at[j - 1, a3],
                        send.at[t, 2], recv.at[t, SE + 4 * (j - 1) + m], moved(axes[t][1], j), core,
                    )

    settle(pxr, xr.at[0])
    olds = []
    for tile in range(4):
        old = jnp.where(hi == 0, pf[:, tile * 128 : tile * 128 + 128], pf[:, 512 + tile * 128 : 640 + tile * 128])
        olds.append((old + pxr[:, tile * 128 : tile * 128 + 128].astype(F32)).astype(BF16))

    def spread(t, buf, ssem, base):
        block = buf[t].at[pos[t][1], pos[t][2]]
        for k in (2, 1, 3):
            push(block, block, send.at[t, ssem], recv.at[t, base + k - 1], moved(axes[t][2], k), core)

    def spread_on(t, buf, ssem, got, base):
        for k in (1, 3, 2):
            settle(buf[t].at[0, 0], recv.at[t, got + k - 1])
        sub = buf[t].at[pos[t][1]]
        for k in (2, 1, 3):
            push(sub, sub, send.at[t, ssem], recv.at[t, base + k - 1], moved(axes[t][1], k), core)

    for t in range(3):
        pg[t][pos[t][1], pos[t][2], 0:56, :] = olds[t]
        pg[t][pos[t][1], pos[t][2], 56 : ROWS[t], :] = olds[3][STRIP[t][0] : STRIP[t][1], :]
        spread(t, pg, 8, PT)

    for m in (2, 1, 3, 0):
        for t in range(3):
            a3 = rel(t, 2, m)
            total = s1[t][0, a3].astype(F32)
            for j in (1, 2, 0):
                settle(r2[t].at[j, a3], recv.at[t, SE + 4 * j + m])
                total = total + r2[t][j, a3].astype(F32)
            if m:
                s2[t][m - 1] = total.astype(BF16)
                push(s2[t].at[m - 1], r3[t].at[m - 1], send.at[t, 3], recv.at[t, TH + m - 1], moved(axes[t][2], m), core)
            else:
                s3[t][...] = total
    for t in range(3):
        spread_on(t, pg, 9, PT, PS)
    for t in range(3):
        total = s3[t][...]
        for m in (0, 2, 1):
            settle(r3[t].at[m], recv.at[t, TH + m])
            total = total + r3[t][m].astype(F32)
        s3[t][...] = total
        sg[t][pos[t][1], pos[t][2]] = total.astype(BF16)

    tiles = [s3[t][0:56, :] for t in range(3)] + [jnp.concatenate([s3[t][56 : ROWS[t], :] for t in range(3)], axis=0)]
    squares = [v * v for v in tiles]
    row_squares = jnp.sum(squares[0] + squares[1] + squares[2] + squares[3], axis=1, keepdims=True)
    sums = [jnp.sum(v, axis=0, keepdims=True) for v in squares]
    mine = at["x"] * 2 + core
    st1[mine] = jnp.concatenate(sums + [rs_row, as_row(row_squares), jnp.zeros((2, 128), F32)], axis=0)
    near_group = [(k, flip) for k in (2, 1, 3, 0) for flip in (1, 0) if k or flip]
    for n, (k, flip) in enumerate(near_group):
        push(st1.at[mine], st1.at[mine], t1s.at[0], t1r.at[n], moved("x", k), 1 - core if flip else core)

    for t in range(3):
        spread(t, sg, 4, GT)

    def added(buf, lo_slot, hi_slot):
        terms = [buf[i] for i in range(lo_slot, hi_slot)]
        while len(terms) > 1:
            terms = [a + b for a, b in zip(terms[0::2], terms[1::2])]
        return terms[0]

    for n in range(7):
        settle(st1.at[0], t1r.at[n])
    slot = at["y"] * 4 + at["z"]
    st2[slot] = added(st1, 0, 8)
    rb[slot] = jnp.concatenate([st1[i, 5:6, :] for i in range(8)] + [st1[i, 4:5, :] for i in range(8)], axis=0)
    far_group = [(i, j) for i in (2, 1, 3, 0) for j in (2, 1, 3, 0) if i or j]
    for buf, ssem, rsem in ((st2, t2s, t2r), (rb, t3s, t3r)):
        for n, (i, j) in enumerate(far_group):
            to = dict(moved("y", i), z=mod4(at["z"] + j))
            push(buf.at[slot], buf.at[slot], ssem.at[0], rsem.at[n], to, core)
    for t in range(3):
        spread_on(t, sg, 5, GT, GS)
    for n in range(15):
        settle(st2.at[0], t2r.at[n])
    half0, half1 = added(st2, 0, 8), added(st2, 8, 16)

    column_sums = jnp.concatenate([half0[0:4, :], half1[0:4, :]], axis=0)
    norm_square = jnp.sum(jnp.sum(column_sums, axis=0, keepdims=True), axis=1, keepdims=True)
    rs_total = jnp.sum(half0[4:5, :] + half1[4:5, :], axis=1, keepdims=True)
    factor = jnp.minimum(1.0, CLIP / jnp.sqrt(norm_square + 1e-06))
    square_factor = factor * factor
    column_next = BETA * cs[...] + (1.0 - BETA) * (square_factor * column_sums * (1.0 / D))
    row_average = (BETA / D) * rs_total + (1.0 - BETA) * (square_factor * norm_square * (1.0 / (D * KW)))
    cf[...] = STEP * factor * jnp.sqrt(row_average) / jnp.sqrt(column_next)
    for n in range(15):
        settle(rb.at[0], t3r.at[n])
    for i in range(8):
        both = rb[i] + rb[8 + i]
        rn[i] = BETA * both[8:16, :] + (1.0 - BETA) * (square_factor * both[0:8, :] * (1.0 / KW))
        rf[i] = 1.0 / jnp.sqrt(rn[i])

    def update(t, j):
        a2 = rel(t, 1, j)

        def body(a3, carry):
            here = {axes[t][0]: pos[t][0], axes[t][1]: a2, axes[t][2]: a3}
            half = 4 * lax.div(here["y"], 2)
            group = lax.rem(here["y"], 2) * 4 + here["z"]
            scale = as_column(rf[group, pl.ds(here["x"] * 2 + core, 1), :])
            new = sg[t][a2, a3].astype(F32)
            old = pg[t][a2, a3].astype(F32)
            own[t][pos[t][0], a2, a3, 0:56, :] = (old[0:56] - new[0:56] * (scale * cf[pl.ds(half + t, 1), :])).astype(BF16)
            own[t][pos[t][0], a2, a3, 56 : ROWS[t], :] = (
                old[56:] - new[56:] * (scale[STRIP[t][0] : STRIP[t][1]] * cf[pl.ds(half + 3, 1), :])
            ).astype(BF16)
            return carry

        lax.fori_loop(0, 4, body, 0)

    def onward(t, block, j):
        push(block, block, send.at[t, 6], recv.at[t, GM + j], moved(axes[t][0], 1), core)
        push(block, block, send.at[t, 6], recv.at[t, GP + j], moved(axes[t][0], 3), core)

    def across(t, a1, a2):
        push(own[t].at[a1, a2], other[t].at[a1, a2], send.at[t, 7], recv.at[t, GC], at, 1 - core)

    for j in (0, 1, 3, 2):
        for t in range(3):
            if j:
                settle(sg[t].at[0], recv.at[t, GS + (4 - j) - 1])
                settle(pg[t].at[0], recv.at[t, PS + (4 - j) - 1])
            update(t, j)
            sub = own[t].at[pos[t][0], rel(t, 1, j)]
            onward(t, sub, j)
            across(t, pos[t][0], rel(t, 1, j))

    for j in (0, 1, 3, 2):
        for t in range(3):
            for base, k, shift in ((GM, 3, 1), (GP, 1, 3)):
                sub = own[t].at[rel(t, 0, k), rel(t, 1, j)]
                settle(sub, recv.at[t, base + j])
                if (j in (0, 3)) == (shift == 1):
                    push(sub, sub, send.at[t, 6], recv.at[t, GO + j], moved(axes[t][0], shift), core)
                across(t, rel(t, 0, k), rel(t, 1, j))
    coln[...] = column_next
    mine_row = rn[lo * 4 + at["z"], pl.ds(mine, 1), :]
    rown[...] = jnp.where(hi == 0, mine_row[:, 0:28], mine_row[:, 28:56])
    for j in (0, 1, 3, 2):
        for t in range(3):
            settle(own[t].at[rel(t, 0, 2), rel(t, 1, j)], recv.at[t, GO + j])
            across(t, rel(t, 0, 2), rel(t, 1, j))

    for h in (0, 1):
        here = dict(at, y=2 * h + lo)
        blocks = [own[t].at[tuple(here[a] for a in axes[t])] for t in range(3)]
        for t in range(3):
            pf[:, 512 * h + 128 * t : 512 * h + 128 * t + 128] = blocks[t][0:56, :].astype(F32)
            pf[STRIP[t][0] : STRIP[t][1], 512 * h + 384 : 512 * h + 512] = blocks[t][56 : ROWS[t], :].astype(F32)
    newp[...] = jnp.where(hi == 0, pf[0:28, :], pf[28:56, :]).astype(BF16)

    for t in range(3):
        settle(w[t], send.at[t, 0])
        settle(w[t].at[0:3], send.at[t, 1])
        settle(w[t].at[0, 0:3], send.at[t, 2])
        settle(w[t].at[0, 0, 0:3], send.at[t, 3])
        settle(w[t].at[0, 0, 0:3], send.at[t, 4])
        settle(w[t].at[0, 0:3], send.at[t, 5])
        settle(w[t].at[0:3], send.at[t, 6])
        settle(w[t], send.at[t, 7])
        settle(w[t].at[0, 0, 0:3], send.at[t, 8])
        settle(w[t].at[0, 0:3], send.at[t, 9])
        settle(other[t], recv.at[t, GC])
    settle(px, xs.at[0])
    settle(st1.at[0:7], t1s.at[0])
    settle(st2.at[0:15], t2s.at[0])
    settle(rb.at[0:15], t3s.at[0])


def layout_kernel(*refs):
    own, other = refs[0:3], refs[3:6]
    newp, rown, coln = refs[6:9]
    whole, newp_out, rown_out, coln_out, sems = refs[9:]
    _, _, _, core = where_am_i()
    for src, dst in ((newp, newp_out), (rown, rown_out), (coln, coln_out)):
        pltpu.make_async_copy(src, dst, sems.at[3]).start()
    for held, c in ((own, core), (other, 1 - core)):
        for t in range(3):
            for a1 in range(4):
                for dst, src in copies(t, a1, c, whole, held[t]):
                    pltpu.make_async_copy(src, dst, sems.at[t]).start()
    for t in range(3):
        for held in (own, other):
            pltpu.make_async_copy(held[t], held[t], sems.at[t]).wait()
    for src, dst in ((newp, newp_out), (rown, rown_out), (coln, coln_out)):
        pltpu.make_async_copy(src, dst, sems.at[3]).wait()


def solution(mesh):
    block = [(r, 128) for r in ROWS]
    part = [jax.ShapeDtypeStruct((4, 4, 4) + b, BF16) for b in block]
    vmem = pl.BlockSpec(memory_space=pltpu.VMEM)
    anywhere = pl.BlockSpec(memory_space=pl.ANY)

    def hbm(v):
        return pltpu.with_memory_space_constraint(v, pltpu.HBM)

    def local(grad_bucket, parameters, row_state, column_state):
        def three(*lead, dtype=BF16):
            return [pltpu.VMEM(lead + b, dtype) for b in block]

        scratch = (
            three(4, 4, 4) + three(4, 4, 4) + three(4, 2) + three(4, 2) + three(4, 4) + three(4, 4) + three(4, 4)
            + three(3, 4) + three(3) + three(3) + three(dtype=F32) + three(4, 4) + three(4, 4)
            + [
                pltpu.VMEM((28, KW), BF16), pltpu.VMEM((1, 28), F32), pltpu.VMEM((8, 128), F32), pltpu.VMEM((8, 128), F32),
                pltpu.VMEM((56, 1024), F32),
                pltpu.VMEM((56, 512), BF16), pltpu.VMEM((56, 512), BF16),
                pltpu.VMEM((8, 8, 128), F32), pltpu.VMEM((16, 8, 128), F32), pltpu.VMEM((16, 16, 128), F32),
                pltpu.VMEM((8, 8, 128), F32), pltpu.VMEM((8, 8, 128), F32), pltpu.VMEM((8, 128), F32),
                pltpu.SemaphoreType.DMA((3, NRECV)), pltpu.SemaphoreType.DMA((3, NSEND)),
                pltpu.SemaphoreType.DMA((1,)), pltpu.SemaphoreType.DMA((1,)),
                pltpu.SemaphoreType.DMA((7,)), pltpu.SemaphoreType.DMA((1,)),
                pltpu.SemaphoreType.DMA((15,)), pltpu.SemaphoreType.DMA((1,)),
                pltpu.SemaphoreType.DMA((15,)), pltpu.SemaphoreType.DMA((1,)),
                pltpu.SemaphoreType.DMA((3,)),
            ]
        )
        small = [
            jax.ShapeDtypeStruct((28, KW), BF16),
            jax.ShapeDtypeStruct((1, 28), F32),
            jax.ShapeDtypeStruct((8, 128), F32),
        ]
        held = pl.pallas_call(
            step_kernel,
            out_shape=part + part + small,
            in_specs=[pl.BlockSpec(memory_space=pltpu.HBM)] * 4,
            out_specs=[vmem] * 9,
            scratch_shapes=scratch,
            compiler_params=pltpu.CompilerParams(
                collective_id=0, has_side_effects=True, vmem_limit_bytes=40 * 1024 * 1024
            ),
            name="adafactor_step",
        )(
            grad_bucket.reshape(4, 2, 2, 4, 56, KW),
            hbm(parameters.reshape(28, KW)),
            hbm(row_state),
            hbm(column_state.reshape(8, 128)),
        )
        whole, newp, rown, coln = pl.pallas_call(
            layout_kernel,
            out_shape=[jax.ShapeDtypeStruct((4, 2, 2, 4, 56, KW), BF16)] + small,
            in_specs=[vmem] * 9,
            out_specs=[anywhere] * 4,
            scratch_shapes=[pltpu.SemaphoreType.DMA((4,))],
            compiler_params=pltpu.CompilerParams(vmem_limit_bytes=20 * 1024 * 1024),
            name="lay_out",
        )(*held)
        return newp.reshape(1, 28, KW), rown, coln.reshape(1, KW), whole.reshape(D, KW)

    every = ("gx", "gy", "gz")
    return jax.shard_map(
        local,
        mesh=mesh,
        in_specs=(P(every, None, None, None), P(None, every, None), P(None, every), P(None, None)),
        out_specs=(P(None, every, None), P(None, every), P(None, None), P(None, None)),
        check_vma=False,
    )
```

```python
import math

import jax
import jax.numpy as jnp
from jax import lax
from jax.experimental import pallas as pl
from jax.experimental.pallas import tpu as pltpu
from jax.sharding import PartitionSpec as P

D = 3584
KW = 1024
CLIP = 0.5 * math.sqrt(D * KW)
BETA = 0.8
STEP = 0.5
MESH = pl.DeviceIdType.MESH
F32 = jnp.float32
BF16 = jnp.bfloat16

ORDER = ("xyz", "yzx", "zxy")
STRIP = ((0, 24), (24, 40), (40, 56))
ROWS = tuple(56 + b - a for a, b in STRIP)
LD, PR, RLP, RLM, FM, FP, SE, TH = 0, 4, 8, 12, 16, 20, 24, 36
GT, GS, GM, GP, GO, GC, PT, PS = 39, 42, 45, 49, 53, 57, 58, 61
NRECV = 64
NSEND = 10


def mod4(v):
    return lax.rem(v, 4)


def where_am_i():
    gx, gy, gz = lax.axis_index("gx"), lax.axis_index("gy"), lax.axis_index("gz")
    lo, core = lax.div(gy, 2), lax.rem(gy, 2)
    z, hi = lax.div(gz, 2), lax.rem(gz, 2)
    return {"x": gx, "y": 2 * hi + lo, "z": z}, lo, hi, core


def device(at, core):
    return (at["x"], lax.rem(at["y"], 2) * 2 + core, at["z"] * 2 + lax.div(at["y"], 2))


def pieces(t, a1):
    every = slice(None)
    if t == 0:
        return [((a1, every, None, every), h, (pl.ds(2 * h, 2), every)) for h in (0, 1)]
    if t == 1:
        hi, lo = lax.div(a1, 2), lax.rem(a1, 2)
        return [((every, lo, None, z), hi, (z, every)) for z in range(4)]
    return [((every, every, None, a1), h, (every, pl.ds(2 * h, 2))) for h in (0, 1)]


def rectangles(t):
    return [(t, 0, 56, 0), (3, STRIP[t][0], STRIP[t][1], 56)]


def copies(t, a1, core, whole, part):
    out = []
    for (x, lo, _, z), h, (i, j) in pieces(t, a1):
        for tile, r0, r1, d0 in rectangles(t):
            col = h * 512 + tile * 128
            if not isinstance(col, int):
                col = pl.multiple_of(col, 128)
            out.append((
                whole.at[x, lo, core, z, pl.ds(r0, r1 - r0), pl.ds(col, 128)],
                part.at[a1, i, j, pl.ds(d0, r1 - r0), :],
            ))
    return out


def step_kernel(*refs):
    (g, par_in, rs_in, cs_in), refs = refs[:4], refs[4:]
    outs, refs = refs[:9], refs[9:]
    own, other = outs[0:3], outs[3:6]
    newp, rown, coln = outs[6:9]
    it = iter(refs)
    take3 = lambda: [next(it) for _ in range(3)]
    w, pr, rlp, rlm, fm, fp, s1, r2, s2, r3, s3, sg, pg = (take3() for _ in range(13))
    par, line, rs, cs, pf, px, pxr, st1, st2, rb, rn, rf, cf = (next(it) for _ in range(13))
    recv, send, xr, xs, t1r, t1s, t2r, t2s, t3r, t3s, near = (next(it) for _ in range(11))

    at, lo, hi, core = where_am_i()

    def moved(axis, k):
        to = dict(at)
        to[axis] = mod4(at[axis] + k)
        return to

    def push(src, dst, ssem, rsem, to, tc):
        pltpu.make_async_remote_copy(
            src_ref=src, dst_ref=dst, send_sem=ssem, recv_sem=rsem, device_id=device(to, tc), device_id_type=MESH
        ).start()

    def settle(ref, sem):
        pltpu.make_async_copy(ref, ref, sem).wait()

    axes = [tuple(ORDER[t]) for t in range(3)]
    pos = [tuple(at[a] for a in axes[t]) for t in range(3)]

    def rel(t, level, k):
        return mod4(pos[t][level] + k)

    small = ((par_in, par), (rs_in, line), (cs_in, cs))
    for i, (src, dst) in enumerate(small):
        pltpu.make_async_copy(src, dst, near.at[i]).start()

    barrier = pltpu.get_barrier_semaphore()
    for axis in "xyz":
        for k in (1, 3):
            pl.semaphore_signal(barrier, inc=1, device_id=device(moved(axis, k), core), device_id_type=MESH)
    pl.semaphore_signal(barrier, inc=1, device_id=device(moved("y", 2), core), device_id_type=MESH)
    pl.semaphore_signal(barrier, inc=1, device_id=device(at, 1 - core), device_id_type=MESH)
    for k in (2,):
        for t in range(3):
            for src, dst in copies(t, rel(t, 0, k), core, g, w[t]):
                pltpu.make_async_copy(src, dst, recv.at[t, LD + k]).start()
    pl.semaphore_wait(barrier, 8)
    for k in (2, 1, 3, 0):
        for t in range(3):
            for src, (_, dst) in zip(
                [s for s, _ in copies(t, rel(t, 0, k), 1 - core, g, pr[t])], copies(t, rel(t, 0, k), core, g, pr[t])
            ):
                push(src, dst, send.at[t, 0], recv.at[t, PR + k], at, 1 - core)
    for k in (1, 3, 0):
        for t in range(3):
            for src, dst in copies(t, rel(t, 0, k), core, g, w[t]):
                pltpu.make_async_copy(src, dst, recv.at[t, LD + k]).start()


    pf[...] = jnp.zeros_like(pf)
    for i, (src, dst) in enumerate(small):
        pltpu.make_async_copy(src, dst, near.at[i]).wait()
    wide = par[...].astype(F32)

    @pl.when(hi == 0)
    def _():
        pf[0:28, :] = wide

    @pl.when(hi == 1)
    def _():
        pf[28:56, :] = wide

    row_of = lax.broadcasted_iota(jnp.int32, (56, 128), 0)
    lane_of = lax.broadcasted_iota(jnp.int32, (56, 128), 1)
    on_diag = row_of == lane_of + 28 * hi
    rs[...] = jnp.zeros_like(rs)
    rs[0:1, 0:28] = line[...]
    rs_row = rs[0:1, :]
    rs_column = jnp.sum(jnp.where(on_diag & (lane_of < 28), jnp.broadcast_to(rs_row, (56, 128)), 0.0), axis=1, keepdims=True)

    def as_row(column):
        return jnp.sum(jnp.where(row_of == lane_of, jnp.broadcast_to(column, (56, 128)), 0.0), axis=0, keepdims=True)

    def as_column(row):
        return jnp.sum(jnp.where(row_of == lane_of, jnp.broadcast_to(row, (56, 128)), 0.0), axis=1, keepdims=True)

    rs_row = jnp.sum(
        jnp.where(row_of == lane_of - 64, jnp.broadcast_to(rs_column, (56, 128)), 0.0), axis=0, keepdims=True
    )
    px[...] = jnp.where(hi == 0, pf[:, 512:1024], pf[:, 0:512]).astype(BF16)
    push(px, pxr, xs.at[0], xr.at[0], moved("y", 2), core)

    def add_chunk(t, a1):
        settle(w[t].at[a1], recv_k[0])
        settle(pr[t].at[a1], recv_k[1])

        def body(i, carry):
            w[t][a1, i] = w[t][a1, i] + pr[t][a1, i]
            return carry

        lax.fori_loop(0, 4, body, 0)

    for k in (2, 1, 3, 0):
        for t in range(3):
            a1 = rel(t, 0, k)
            recv_k = (recv.at[t, LD + k], recv.at[t, PR + k])
            add_chunk(t, a1)
            up, down = moved(axes[t][0], 1), moved(axes[t][0], 3)
            if k == 2:
                for j in (2, 3, 1, 0):
                    sub = w[t].at[a1, rel(t, 1, j)]
                    push(sub.at[0:2], rlp[t].at[j], send.at[t, 1], recv.at[t, RLP + j], up, core)
                    push(sub.at[2:4], rlm[t].at[j], send.at[t, 1], recv.at[t, RLM + j], down, core)
            if k == 1:
                for j in (2, 3, 1, 0):
                    sub = w[t].at[a1, rel(t, 1, j)]
                    push(sub.at[2:4], fm[t].at[j, 2:4], send.at[t, 1], recv.at[t, FM + j], up, core)
            if k == 3:
                for j in (2, 3, 1, 0):
                    sub = w[t].at[a1, rel(t, 1, j)]
                    push(sub.at[0:2], fp[t].at[j, 0:2], send.at[t, 1], recv.at[t, FP + j], down, core)

    for j in (2, 3, 1, 0):
        for t in range(3):
            up, down = moved(axes[t][0], 1), moved(axes[t][0], 3)
            for k, half, buf, base, dst, dbase, to in (
                (1, 0, rlp[t], RLP, fm[t], FM, up),
                (3, 2, rlm[t], RLM, fp[t], FP, down),
            ):
                settle(buf.at[j], recv.at[t, base + j])
                a1, a2 = rel(t, 0, k), rel(t, 1, j)
                w[t][a1, a2, half : half + 2] = w[t][a1, a2, half : half + 2] + buf[j]
                push(
                    w[t].at[a1, a2, half : half + 2], dst.at[j, half : half + 2],
                    send.at[t, 1], recv.at[t, dbase + j], to, core,
                )

    for j in (2, 3, 1, 0):
        for t in range(3):
            settle(fm[t].at[j], recv.at[t, FM + j])
            settle(fp[t].at[j], recv.at[t, FP + j])
            a1, a2 = rel(t, 0, 0), rel(t, 1, j)
            for m in (2, 1, 3, 0):
                a3 = rel(t, 2, m)
                s1[t][j, a3] = (
                    w[t][a1, a2, a3].astype(F32) + fm[t][j, a3].astype(F32) + fp[t][j, a3].astype(F32)
                ).astype(BF16)
                if j:
                    push(
                        s1[t].at[j, a3], r2[t].at[j - 1, a3],
                        send.at[t, 2], recv.at[t, SE + 4 * (j - 1) + m], moved(axes[t][1], j), core,
                    )

    settle(pxr, xr.at[0])
    olds = []
    for tile in range(4):
        old = jnp.where(hi == 0, pf[:, tile * 128 : tile * 128 + 128], pf[:, 512 + tile * 128 : 640 + tile * 128])
        olds.append((old + pxr[:, tile * 128 : tile * 128 + 128].astype(F32)).astype(BF16))

    def spread(t, buf, ssem, base):
        block = buf[t].at[pos[t][1], pos[t][2]]
        for k in (2, 1, 3):
            push(block, block, send.at[t, ssem], recv.at[t, base + k - 1], moved(axes[t][2], k), core)

    def spread_on(t, buf, ssem, got, base):
        for k in (1, 3, 2):
            settle(buf[t].at[0, 0], recv.at[t, got + k - 1])
        sub = buf[t].at[pos[t][1]]
        for k in (2, 1, 3):
            push(sub, sub, send.at[t, ssem], recv.at[t, base + k - 1], moved(axes[t][1], k), core)

    for t in range(3):
        pg[t][pos[t][1], pos[t][2], 0:56, :] = olds[t]
        pg[t][pos[t][1], pos[t][2], 56 : ROWS[t], :] = olds[3][STRIP[t][0] : STRIP[t][1], :]
        spread(t, pg, 8, PT)

    for m in (2, 1, 3, 0):
        for t in range(3):
            a3 = rel(t, 2, m)
            total = s1[t][0, a3].astype(F32)
            for j in (1, 2, 0):
                settle(r2[t].at[j, a3], recv.at[t, SE + 4 * j + m])
                total = total + r2[t][j, a3].astype(F32)
            if m:
                s2[t][m - 1] = total.astype(BF16)
                push(s2[t].at[m - 1], r3[t].at[m - 1], send.at[t, 3], recv.at[t, TH + m - 1], moved(axes[t][2], m), core)
            else:
                s3[t][...] = total
    for t in range(3):
        total = s3[t][...]
        for m in (0, 2, 1):
            settle(r3[t].at[m], recv.at[t, TH + m])
            total = total + r3[t][m].astype(F32)
        s3[t][...] = total
        sg[t][pos[t][1], pos[t][2]] = total.astype(BF16)

    tiles = [s3[t][0:56, :] for t in range(3)] + [jnp.concatenate([s3[t][56 : ROWS[t], :] for t in range(3)], axis=0)]
    squares = [v * v for v in tiles]
    row_squares = jnp.sum(squares[0] + squares[1] + squares[2] + squares[3], axis=1, keepdims=True)
    sums = [jnp.sum(v, axis=0, keepdims=True) for v in squares]
    mine = at["x"] * 2 + core
    st1[mine] = jnp.concatenate(sums + [rs_row, as_row(row_squares) + rs_row, jnp.zeros((2, 128), F32)], axis=0)
    near_group = [(k, flip) for k in (2, 1, 3, 0) for flip in (1, 0) if k or flip]
    for n, (k, flip) in enumerate(near_group):
        push(st1.at[mine], st1.at[mine], t1s.at[0], t1r.at[n], moved("x", k), 1 - core if flip else core)

    for t in range(3):
        spread(t, sg, 4, GT)
    for t in range(3):
        spread_on(t, pg, 9, PT, PS)

    def added(buf, lo_slot, hi_slot):
        terms = [buf[i] for i in range(lo_slot, hi_slot)]
        while len(terms) > 1:
            terms = [a + b for a, b in zip(terms[0::2], terms[1::2])]
        return terms[0]

    for n in range(7):
        settle(st1.at[0], t1r.at[n])
    slot = at["y"] * 4 + at["z"]
    st2[slot] = added(st1, 0, 8)
    rb[slot] = jnp.concatenate([st1[i, 5:6, :] for i in range(8)], axis=0)
    far_group = [(i, j) for i in (2, 1, 3, 0) for j in (2, 1, 3, 0) if i or j]
    for buf, ssem, rsem in ((st2, t2s, t2r), (rb, t3s, t3r)):
        for n, (i, j) in enumerate(far_group):
            to = dict(moved("y", i), z=mod4(at["z"] + j))
            push(buf.at[slot], buf.at[slot], ssem.at[0], rsem.at[n], to, core)
    for t in range(3):
        spread_on(t, sg, 5, GT, GS)
    for n in range(15):
        settle(st2.at[0], t2r.at[n])
    half0, half1 = added(st2, 0, 8), added(st2, 8, 16)

    column_sums = jnp.concatenate([half0[0:4, :], half1[0:4, :]], axis=0)
    norm_square = jnp.sum(jnp.sum(column_sums, axis=0, keepdims=True), axis=1, keepdims=True)
    rs_total = jnp.sum(half0[4:5, :] + half1[4:5, :], axis=1, keepdims=True)
    factor = jnp.minimum(1.0, CLIP / jnp.sqrt(norm_square + 1e-06))
    square_factor = factor * factor
    column_next = BETA * cs[...] + (1.0 - BETA) * (square_factor * column_sums * (1.0 / D))
    row_average = (BETA / D) * rs_total + (1.0 - BETA) * (square_factor * norm_square * (1.0 / (D * KW)))
    cf[...] = STEP * factor * jnp.sqrt(row_average) / jnp.sqrt(column_next)
    for n in range(15):
        settle(rb.at[0], t3r.at[n])
    for i in range(8):
        both = rb[i] + rb[8 + i]
        rn[i] = BETA * pltpu.roll(both, 64, 1) + (1.0 - BETA) * (square_factor * both * (1.0 / KW))
        rf[i] = 1.0 / jnp.sqrt(rn[i])

    def update(t, j):
        a2 = rel(t, 1, j)

        def body(a3, carry):
            here = {axes[t][0]: pos[t][0], axes[t][1]: a2, axes[t][2]: a3}
            half = 4 * lax.div(here["y"], 2)
            group = lax.rem(here["y"], 2) * 4 + here["z"]
            scale = as_column(rf[group, pl.ds(here["x"] * 2 + core, 1), :])
            new = sg[t][a2, a3].astype(F32)
            old = pg[t][a2, a3].astype(F32)
            own[t][pos[t][0], a2, a3, 0:56, :] = (old[0:56] - new[0:56] * (scale * cf[pl.ds(half + t, 1), :])).astype(BF16)
            own[t][pos[t][0], a2, a3, 56 : ROWS[t], :] = (
                old[56:] - new[56:] * (scale[STRIP[t][0] : STRIP[t][1]] * cf[pl.ds(half + 3, 1), :])
            ).astype(BF16)
            return carry

        lax.fori_loop(0, 4, body, 0)

    def onward(t, block, j):
        push(block, block, send.at[t, 6], recv.at[t, GM + j], moved(axes[t][0], 1), core)
        push(block, block, send.at[t, 6], recv.at[t, GP + j], moved(axes[t][0], 3), core)

    def across(t, a1, a2):
        push(own[t].at[a1, a2], other[t].at[a1, a2], send.at[t, 7], recv.at[t, GC], at, 1 - core)

    for j in (0, 1, 3, 2):
        for t in range(3):
            if j:
                settle(sg[t].at[0], recv.at[t, GS + (4 - j) - 1])
                settle(pg[t].at[0], recv.at[t, PS + (4 - j) - 1])
            update(t, j)
            sub = own[t].at[pos[t][0], rel(t, 1, j)]
            onward(t, sub, j)
            across(t, pos[t][0], rel(t, 1, j))

    for j in (0, 1, 3, 2):
        for t in range(3):
            for base, k, shift in ((GM, 3, 1), (GP, 1, 3)):
                sub = own[t].at[rel(t, 0, k), rel(t, 1, j)]
                settle(sub, recv.at[t, base + j])
                if (j in (0, 3)) == (shift == 1):
                    push(sub, sub, send.at[t, 6], recv.at[t, GO + j], moved(axes[t][0], shift), core)
                across(t, rel(t, 0, k), rel(t, 1, j))
    coln[...] = column_next
    mine_row = rn[lo * 4 + at["z"], pl.ds(mine, 1), :]
    rown[...] = jnp.where(hi == 0, mine_row[:, 0:28], mine_row[:, 28:56])
    for j in (0, 1, 3, 2):
        for t in range(3):
            settle(own[t].at[rel(t, 0, 2), rel(t, 1, j)], recv.at[t, GO + j])
            across(t, rel(t, 0, 2), rel(t, 1, j))

    for h in (0, 1):
        here = dict(at, y=2 * h + lo)
        blocks = [own[t].at[tuple(here[a] for a in axes[t])] for t in range(3)]
        for t in range(3):
            pf[:, 512 * h + 128 * t : 512 * h + 128 * t + 128] = blocks[t][0:56, :].astype(F32)
            pf[STRIP[t][0] : STRIP[t][1], 512 * h + 384 : 512 * h + 512] = blocks[t][56 : ROWS[t], :].astype(F32)
    newp[...] = jnp.where(hi == 0, pf[0:28, :], pf[28:56, :]).astype(BF16)

    for t in range(3):
        settle(w[t], send.at[t, 0])
        settle(w[t].at[0:3], send.at[t, 1])
        settle(w[t].at[0, 0:3], send.at[t, 2])
        settle(w[t].at[0, 0, 0:3], send.at[t, 3])
        settle(w[t].at[0, 0, 0:3], send.at[t, 4])
        settle(w[t].at[0, 0:3], send.at[t, 5])
        settle(w[t].at[0:3], send.at[t, 6])
        settle(w[t], send.at[t, 7])
        settle(w[t].at[0, 0, 0:3], send.at[t, 8])
        settle(w[t].at[0, 0:3], send.at[t, 9])
        settle(other[t], recv.at[t, GC])
    settle(px, xs.at[0])
    settle(st1.at[0:7], t1s.at[0])
    settle(st2.at[0:15], t2s.at[0])
    settle(rb.at[0:15], t3s.at[0])


def layout_kernel(*refs):
    own, other = refs[0:3], refs[3:6]
    newp, rown, coln = refs[6:9]
    whole, newp_out, rown_out, coln_out, sems = refs[9:]
    _, _, _, core = where_am_i()
    for src, dst in ((newp, newp_out), (rown, rown_out), (coln, coln_out)):
        pltpu.make_async_copy(src, dst, sems.at[3]).start()
    for held, c in ((own, core), (other, 1 - core)):
        for t in range(3):
            for a1 in range(4):
                for dst, src in copies(t, a1, c, whole, held[t]):
                    pltpu.make_async_copy(src, dst, sems.at[t]).start()
    for t in range(3):
        for held in (own, other):
            pltpu.make_async_copy(held[t], held[t], sems.at[t]).wait()
    for src, dst in ((newp, newp_out), (rown, rown_out), (coln, coln_out)):
        pltpu.make_async_copy(src, dst, sems.at[3]).wait()


def solution(mesh):
    block = [(r, 128) for r in ROWS]
    part = [jax.ShapeDtypeStruct((4, 4, 4) + b, BF16) for b in block]
    vmem = pl.BlockSpec(memory_space=pltpu.VMEM)
    anywhere = pl.BlockSpec(memory_space=pl.ANY)

    def hbm(v):
        return pltpu.with_memory_space_constraint(v, pltpu.HBM)

    def local(grad_bucket, parameters, row_state, column_state):
        def three(*lead, dtype=BF16):
            return [pltpu.VMEM(lead + b, dtype) for b in block]

        scratch = (
            three(4, 4, 4) + three(4, 4, 4) + three(4, 2) + three(4, 2) + three(4, 4) + three(4, 4) + three(4, 4)
            + three(3, 4) + three(3) + three(3) + three(dtype=F32) + three(4, 4) + three(4, 4)
            + [
                pltpu.VMEM((28, KW), BF16), pltpu.VMEM((1, 28), F32), pltpu.VMEM((8, 128), F32), pltpu.VMEM((8, 128), F32),
                pltpu.VMEM((56, 1024), F32),
                pltpu.VMEM((56, 512), BF16), pltpu.VMEM((56, 512), BF16),
                pltpu.VMEM((8, 8, 128), F32), pltpu.VMEM((16, 8, 128), F32), pltpu.VMEM((16, 8, 128), F32),
                pltpu.VMEM((8, 8, 128), F32), pltpu.VMEM((8, 8, 128), F32), pltpu.VMEM((8, 128), F32),
                pltpu.SemaphoreType.DMA((3, NRECV)), pltpu.SemaphoreType.DMA((3, NSEND)),
                pltpu.SemaphoreType.DMA((1,)), pltpu.SemaphoreType.DMA((1,)),
                pltpu.SemaphoreType.DMA((7,)), pltpu.SemaphoreType.DMA((1,)),
                pltpu.SemaphoreType.DMA((15,)), pltpu.SemaphoreType.DMA((1,)),
                pltpu.SemaphoreType.DMA((15,)), pltpu.SemaphoreType.DMA((1,)),
                pltpu.SemaphoreType.DMA((3,)),
            ]
        )
        small = [
            jax.ShapeDtypeStruct((28, KW), BF16),
            jax.ShapeDtypeStruct((1, 28), F32),
            jax.ShapeDtypeStruct((8, 128), F32),
        ]
        held = pl.pallas_call(
            step_kernel,
            out_shape=part + part + small,
            in_specs=[pl.BlockSpec(memory_space=pltpu.HBM)] * 4,
            out_specs=[vmem] * 9,
            scratch_shapes=scratch,
            compiler_params=pltpu.CompilerParams(
                collective_id=0, has_side_effects=True, vmem_limit_bytes=40 * 1024 * 1024
            ),
            name="adafactor_step",
        )(
            grad_bucket.reshape(4, 2, 2, 4, 56, KW),
            hbm(parameters.reshape(28, KW)),
            hbm(row_state),
            hbm(column_state.reshape(8, 128)),
        )
        whole, newp, rown, coln = pl.pallas_call(
            layout_kernel,
            out_shape=[jax.ShapeDtypeStruct((4, 2, 2, 4, 56, KW), BF16)] + small,
            in_specs=[vmem] * 9,
            out_specs=[anywhere] * 4,
            scratch_shapes=[pltpu.SemaphoreType.DMA((4,))],
            compiler_params=pltpu.CompilerParams(vmem_limit_bytes=20 * 1024 * 1024),
            name="lay_out",
        )(*held)
        return newp.reshape(1, 28, KW), rown, coln.reshape(1, KW), whole.reshape(D, KW)

    every = ("gx", "gy", "gz")
    return jax.shard_map(
        local,
        mesh=mesh,
        in_specs=(P(every, None, None, None), P(None, every, None), P(None, every), P(None, None)),
        out_specs=(P(None, every, None), P(None, every), P(None, None), P(None, None)),
        check_vma=False,
    )
```

```python
import math

import jax
import jax.numpy as jnp
from jax import lax
from jax.experimental import pallas as pl
from jax.experimental.pallas import tpu as pltpu
from jax.sharding import PartitionSpec as P

D = 3584
KW = 1024
CLIP = 0.5 * math.sqrt(D * KW)
BETA = 0.8
STEP = 0.5
MESH = pl.DeviceIdType.MESH
F32 = jnp.float32
BF16 = jnp.bfloat16

ORDER = ("xyz", "yzx", "zxy")
STRIP = ((0, 24), (24, 40), (40, 56))
ROWS = tuple(56 + b - a for a, b in STRIP)
LD, PR, RLP, RLM, FM, FP, SE, TH = 0, 4, 8, 12, 16, 20, 24, 36
GT, GS, GM, GP, GO, GC, PT, PS = 39, 42, 45, 49, 53, 57, 58, 61
NRECV = 64
NSEND = 10


def mod4(v):
    return lax.rem(v, 4)


def where_am_i():
    gx, gy, gz = lax.axis_index("gx"), lax.axis_index("gy"), lax.axis_index("gz")
    lo, core = lax.div(gy, 2), lax.rem(gy, 2)
    z, hi = lax.div(gz, 2), lax.rem(gz, 2)
    return {"x": gx, "y": 2 * hi + lo, "z": z}, lo, hi, core


def device(at, core):
    return (at["x"], lax.rem(at["y"], 2) * 2 + core, at["z"] * 2 + lax.div(at["y"], 2))


def pieces(t, a1):
    every = slice(None)
    if t == 0:
        return [((a1, every, None, every), h, (pl.ds(2 * h, 2), every)) for h in (0, 1)]
    if t == 1:
        hi, lo = lax.div(a1, 2), lax.rem(a1, 2)
        return [((every, lo, None, z), hi, (z, every)) for z in range(4)]
    return [((every, every, None, a1), h, (every, pl.ds(2 * h, 2))) for h in (0, 1)]


def rectangles(t):
    return [(t, 0, 56, 0), (3, STRIP[t][0], STRIP[t][1], 56)]


def copies(t, a1, core, whole, part):
    out = []
    for (x, lo, _, z), h, (i, j) in pieces(t, a1):
        for tile, r0, r1, d0 in rectangles(t):
            col = h * 512 + tile * 128
            if not isinstance(col, int):
                col = pl.multiple_of(col, 128)
            out.append((
                whole.at[x, lo, core, z, pl.ds(r0, r1 - r0), pl.ds(col, 128)],
                part.at[a1, i, j, pl.ds(d0, r1 - r0), :],
            ))
    return out


def step_kernel(*refs):
    (g, par_in, rs_in, cs_in), refs = refs[:4], refs[4:]
    outs, refs = refs[:9], refs[9:]
    own, other = outs[0:3], outs[3:6]
    newp, rown, coln = outs[6:9]
    it = iter(refs)
    take3 = lambda: [next(it) for _ in range(3)]
    w, pr, rlp, rlm, fm, fp, s1, r2, s2, r3, s3, sg, pg = (take3() for _ in range(13))
    par, line, rs, cs, pf, px, pxr, st1, st2, rb, rn, rf, cf = (next(it) for _ in range(13))
    recv, send, xr, xs, t1r, t1s, t2r, t2s, t3r, t3s, near = (next(it) for _ in range(11))

    at, lo, hi, core = where_am_i()

    def moved(axis, k):
        to = dict(at)
        to[axis] = mod4(at[axis] + k)
        return to

    def push(src, dst, ssem, rsem, to, tc):
        pltpu.make_async_remote_copy(
            src_ref=src, dst_ref=dst, send_sem=ssem, recv_sem=rsem, device_id=device(to, tc), device_id_type=MESH
        ).start()

    def settle(ref, sem):
        pltpu.make_async_copy(ref, ref, sem).wait()

    axes = [tuple(ORDER[t]) for t in range(3)]
    pos = [tuple(at[a] for a in axes[t]) for t in range(3)]

    def rel(t, level, k):
        return mod4(pos[t][level] + k)

    small = ((par_in, par), (rs_in, line), (cs_in, cs))
    for i, (src, dst) in enumerate(small):
        pltpu.make_async_copy(src, dst, near.at[i]).start()

    barrier = pltpu.get_barrier_semaphore()
    for axis in "xyz":
        for k in (1, 3):
            pl.semaphore_signal(barrier, inc=1, device_id=device(moved(axis, k), core), device_id_type=MESH)
    pl.semaphore_signal(barrier, inc=1, device_id=device(moved("y", 2), core), device_id_type=MESH)
    pl.semaphore_signal(barrier, inc=1, device_id=device(at, 1 - core), device_id_type=MESH)
    for k in (2,):
        for t in range(3):
            for src, dst in copies(t, rel(t, 0, k), core, g, w[t]):
                pltpu.make_async_copy(src, dst, recv.at[t, LD + k]).start()
    pl.semaphore_wait(barrier, 8)
    for k in (2, 1, 3, 0):
        for t in range(3):
            for src, (_, dst) in zip(
                [s for s, _ in copies(t, rel(t, 0, k), 1 - core, g, pr[t])], copies(t, rel(t, 0, k), core, g, pr[t])
            ):
                push(src, dst, send.at[t, 0], recv.at[t, PR + k], at, 1 - core)
    for k in (1, 3, 0):
        for t in range(3):
            for src, dst in copies(t, rel(t, 0, k), core, g, w[t]):
                pltpu.make_async_copy(src, dst, recv.at[t, LD + k]).start()


    pf[...] = jnp.zeros_like(pf)
    for i, (src, dst) in enumerate(small):
        pltpu.make_async_copy(src, dst, near.at[i]).wait()
    wide = par[...].astype(F32)

    @pl.when(hi == 0)
    def _():
        pf[0:28, :] = wide

    @pl.when(hi == 1)
    def _():
        pf[28:56, :] = wide

    row_of = lax.broadcasted_iota(jnp.int32, (56, 128), 0)
    lane_of = lax.broadcasted_iota(jnp.int32, (56, 128), 1)
    on_diag = row_of == lane_of + 28 * hi
    rs[...] = jnp.zeros_like(rs)
    rs[0:1, 0:28] = line[...]
    rs_row = rs[0:1, :]
    rs_column = jnp.sum(jnp.where(on_diag & (lane_of < 28), jnp.broadcast_to(rs_row, (56, 128)), 0.0), axis=1, keepdims=True)

    def as_row(column):
        return jnp.sum(jnp.where(row_of == lane_of, jnp.broadcast_to(column, (56, 128)), 0.0), axis=0, keepdims=True)

    def as_column(row):
        return jnp.sum(jnp.where(row_of == lane_of, jnp.broadcast_to(row, (56, 128)), 0.0), axis=1, keepdims=True)

    rs_row = jnp.sum(
        jnp.where(row_of == lane_of - 64, jnp.broadcast_to(rs_column, (56, 128)), 0.0), axis=0, keepdims=True
    )
    px[...] = jnp.where(hi == 0, pf[:, 512:1024], pf[:, 0:512]).astype(BF16)
    push(px, pxr, xs.at[0], xr.at[0], moved("y", 2), core)

    def add_chunk(t, a1):
        settle(w[t].at[a1], recv_k[0])
        settle(pr[t].at[a1], recv_k[1])

        def body(i, carry):
            w[t][a1, i] = w[t][a1, i] + pr[t][a1, i]
            return carry

        lax.fori_loop(0, 4, body, 0)

    for k in (2, 1, 3, 0):
        for t in range(3):
            a1 = rel(t, 0, k)
            recv_k = (recv.at[t, LD + k], recv.at[t, PR + k])
            add_chunk(t, a1)
            up, down = moved(axes[t][0], 1), moved(axes[t][0], 3)
            if k == 2:
                for j in (2, 3, 1, 0):
                    sub = w[t].at[a1, rel(t, 1, j)]
                    push(sub.at[0:2], rlp[t].at[j], send.at[t, 1], recv.at[t, RLP + j], up, core)
                    push(sub.at[2:4], rlm[t].at[j], send.at[t, 1], recv.at[t, RLM + j], down, core)
            if k == 1:
                for j in (2, 3, 1, 0):
                    sub = w[t].at[a1, rel(t, 1, j)]
                    push(sub.at[2:4], fm[t].at[j, 2:4], send.at[t, 1], recv.at[t, FM + j], up, core)
            if k == 3:
                for j in (2, 3, 1, 0):
                    sub = w[t].at[a1, rel(t, 1, j)]
                    push(sub.at[0:2], fp[t].at[j, 0:2], send.at[t, 1], recv.at[t, FP + j], down, core)

    for j in (2, 3, 1, 0):
        for t in range(3):
            up, down = moved(axes[t][0], 1), moved(axes[t][0], 3)
            for k, half, buf, base, dst, dbase, to in (
                (1, 0, rlp[t], RLP, fm[t], FM, up),
                (3, 2, rlm[t], RLM, fp[t], FP, down),
            ):
                settle(buf.at[j], recv.at[t, base + j])
                a1, a2 = rel(t, 0, k), rel(t, 1, j)
                w[t][a1, a2, half : half + 2] = w[t][a1, a2, half : half + 2] + buf[j]
                push(
                    w[t].at[a1, a2, half : half + 2], dst.at[j, half : half + 2],
                    send.at[t, 1], recv.at[t, dbase + j], to, core,
                )

    for j in (2, 3, 1, 0):
        for t in range(3):
            settle(fm[t].at[j], recv.at[t, FM + j])
            settle(fp[t].at[j], recv.at[t, FP + j])
            a1, a2 = rel(t, 0, 0), rel(t, 1, j)
            for m in (2, 1, 3, 0):
                a3 = rel(t, 2, m)
                s1[t][j, a3] = (
                    w[t][a1, a2, a3].astype(F32) + fm[t][j, a3].astype(F32) + fp[t][j, a3].astype(F32)
                ).astype(BF16)
                if j:
                    push(
                        s1[t].at[j, a3], r2[t].at[j - 1, a3],
                        send.at[t, 2], recv.at[t, SE + 4 * (j - 1) + m], moved(axes[t][1], j), core,
                    )

    settle(pxr, xr.at[0])
    olds = []
    for tile in range(4):
        old = jnp.where(hi == 0, pf[:, tile * 128 : tile * 128 + 128], pf[:, 512 + tile * 128 : 640 + tile * 128])
        olds.append((old + pxr[:, tile * 128 : tile * 128 + 128].astype(F32)).astype(BF16))

    def spread(t, buf, ssem, base):
        block = buf[t].at[pos[t][1], pos[t][2]]
        for k in (2, 1, 3):
            push(block, block, send.at[t, ssem], recv.at[t, base + k - 1], moved(axes[t][2], k), core)

    def spread_on(t, buf, ssem, got, base):
        for k in (1, 3, 2):
            settle(buf[t].at[0, 0], recv.at[t, got + k - 1])
        sub = buf[t].at[pos[t][1]]
        for k in (1, 3, 2):
            push(sub, sub, send.at[t, ssem], recv.at[t, base + k - 1], moved(axes[t][1], k), core)

    for t in range(3):
        pg[t][pos[t][1], pos[t][2], 0:56, :] = olds[t]
        pg[t][pos[t][1], pos[t][2], 56 : ROWS[t], :] = olds[3][STRIP[t][0] : STRIP[t][1], :]
        spread(t, pg, 8, PT)

    for m in (2, 1, 3, 0):
        for t in range(3):
            a3 = rel(t, 2, m)
            total = s1[t][0, a3].astype(F32)
            for j in (1, 2, 0):
                settle(r2[t].at[j, a3], recv.at[t, SE + 4 * j + m])
                total = total + r2[t][j, a3].astype(F32)
            if m:
                s2[t][m - 1] = total.astype(BF16)
                push(s2[t].at[m - 1], r3[t].at[m - 1], send.at[t, 3], recv.at[t, TH + m - 1], moved(axes[t][2], m), core)
            else:
                s3[t][...] = total
    for t in range(3):
        total = s3[t][...]
        for m in (0, 2, 1):
            settle(r3[t].at[m], recv.at[t, TH + m])
            total = total + r3[t][m].astype(F32)
        s3[t][...] = total
        sg[t][pos[t][1], pos[t][2]] = total.astype(BF16)

    tiles = [s3[t][0:56, :] for t in range(3)] + [jnp.concatenate([s3[t][56 : ROWS[t], :] for t in range(3)], axis=0)]
    squares = [v * v for v in tiles]
    row_squares = jnp.sum(squares[0] + squares[1] + squares[2] + squares[3], axis=1, keepdims=True)
    sums = [jnp.sum(v, axis=0, keepdims=True) for v in squares]
    mine = at["x"] * 2 + core
    st1[mine] = jnp.concatenate(sums + [rs_row, as_row(row_squares) + rs_row, jnp.zeros((2, 128), F32)], axis=0)
    near_group = [(k, flip) for k in (2, 1, 3, 0) for flip in (1, 0) if k or flip]
    for n, (k, flip) in enumerate(near_group):
        push(st1.at[mine], st1.at[mine], t1s.at[0], t1r.at[n], moved("x", k), 1 - core if flip else core)

    for t in range(3):
        spread(t, sg, 4, GT)
    for t in range(3):
        spread_on(t, pg, 9, PT, PS)

    def added(buf, lo_slot, hi_slot):
        terms = [buf[i] for i in range(lo_slot, hi_slot)]
        while len(terms) > 1:
            terms = [a + b for a, b in zip(terms[0::2], terms[1::2])]
        return terms[0]

    for n in range(7):
        settle(st1.at[0], t1r.at[n])
    slot = at["y"] * 4 + at["z"]
    st2[slot] = added(st1, 0, 8)
    rb[slot] = jnp.concatenate([st1[i, 5:6, :] for i in range(8)], axis=0)
    far_group = [(i, j) for i in (2, 1, 3, 0) for j in (2, 1, 3, 0) if i or j]
    for buf, ssem, rsem in ((st2, t2s, t2r), (rb, t3s, t3r)):
        for n, (i, j) in enumerate(far_group):
            to = dict(moved("y", i), z=mod4(at["z"] + j))
            push(buf.at[slot], buf.at[slot], ssem.at[0], rsem.at[n], to, core)
    for t in range(3):
        spread_on(t, sg, 5, GT, GS)
    for n in range(15):
        settle(st2.at[0], t2r.at[n])
    half0, half1 = added(st2, 0, 8), added(st2, 8, 16)

    column_sums = jnp.concatenate([half0[0:4, :], half1[0:4, :]], axis=0)
    norm_square = jnp.sum(jnp.sum(column_sums, axis=0, keepdims=True), axis=1, keepdims=True)
    rs_total = jnp.sum(half0[4:5, :] + half1[4:5, :], axis=1, keepdims=True)
    factor = jnp.minimum(1.0, CLIP / jnp.sqrt(norm_square + 1e-06))
    square_factor = factor * factor
    column_next = BETA * cs[...] + (1.0 - BETA) * (square_factor * column_sums * (1.0 / D))
    row_average = (BETA / D) * rs_total + (1.0 - BETA) * (square_factor * norm_square * (1.0 / (D * KW)))
    cf[...] = STEP * factor * jnp.sqrt(row_average) / jnp.sqrt(column_next)
    for n in range(15):
        settle(rb.at[0], t3r.at[n])
    for i in range(8):
        both = rb[i] + rb[8 + i]
        rn[i] = BETA * pltpu.roll(both, 64, 1) + (1.0 - BETA) * (square_factor * both * (1.0 / KW))
        rf[i] = 1.0 / jnp.sqrt(rn[i])

    def update(t, j):
        a2 = rel(t, 1, j)

        def body(a3, carry):
            here = {axes[t][0]: pos[t][0], axes[t][1]: a2, axes[t][2]: a3}
            half = 4 * lax.div(here["y"], 2)
            group = lax.rem(here["y"], 2) * 4 + here["z"]
            scale = as_column(rf[group, pl.ds(here["x"] * 2 + core, 1), :])
            new = sg[t][a2, a3].astype(F32)
            old = pg[t][a2, a3].astype(F32)
            own[t][pos[t][0], a2, a3, 0:56, :] = (old[0:56] - new[0:56] * (scale * cf[pl.ds(half + t, 1), :])).astype(BF16)
            own[t][pos[t][0], a2, a3, 56 : ROWS[t], :] = (
                old[56:] - new[56:] * (scale[STRIP[t][0] : STRIP[t][1]] * cf[pl.ds(half + 3, 1), :])
            ).astype(BF16)
            return carry

        lax.fori_loop(0, 4, body, 0)

    def onward(t, block, j):
        push(block, block, send.at[t, 6], recv.at[t, GM + j], moved(axes[t][0], 1), core)
        push(block, block, send.at[t, 6], recv.at[t, GP + j], moved(axes[t][0], 3), core)

    def across(t, a1, a2):
        push(own[t].at[a1, a2], other[t].at[a1, a2], send.at[t, 7], recv.at[t, GC], at, 1 - core)

    for j in (0, 1, 3, 2):
        for t in range(3):
            if j:
                settle(sg[t].at[0], recv.at[t, GS + (4 - j) - 1])
                settle(pg[t].at[0], recv.at[t, PS + (4 - j) - 1])
            update(t, j)
            sub = own[t].at[pos[t][0], rel(t, 1, j)]
            onward(t, sub, j)
            if j == 2:
                push(own[t].at[pos[t][0]], other[t].at[pos[t][0]], send.at[t, 7], recv.at[t, GC], at, 1 - core)

    for j in (0, 1, 3, 2):
        for t in range(3):
            for base, k, shift in ((GM, 3, 1), (GP, 1, 3)):
                sub = own[t].at[rel(t, 0, k), rel(t, 1, j)]
                settle(sub, recv.at[t, base + j])
                if (j in (0, 3)) == (shift == 1):
                    push(sub, sub, send.at[t, 6], recv.at[t, GO + j], moved(axes[t][0], shift), core)
                across(t, rel(t, 0, k), rel(t, 1, j))
    coln[...] = column_next
    mine_row = rn[lo * 4 + at["z"], pl.ds(mine, 1), :]
    rown[...] = jnp.where(hi == 0, mine_row[:, 0:28], mine_row[:, 28:56])
    for j in (0, 1, 3, 2):
        for t in range(3):
            settle(own[t].at[rel(t, 0, 2), rel(t, 1, j)], recv.at[t, GO + j])
            across(t, rel(t, 0, 2), rel(t, 1, j))

    for h in (0, 1):
        here = dict(at, y=2 * h + lo)
        blocks = [own[t].at[tuple(here[a] for a in axes[t])] for t in range(3)]
        for t in range(3):
            pf[:, 512 * h + 128 * t : 512 * h + 128 * t + 128] = blocks[t][0:56, :].astype(F32)
            pf[STRIP[t][0] : STRIP[t][1], 512 * h + 384 : 512 * h + 512] = blocks[t][56 : ROWS[t], :].astype(F32)
    newp[...] = jnp.where(hi == 0, pf[0:28, :], pf[28:56, :]).astype(BF16)

    for t in range(3):
        settle(w[t], send.at[t, 0])
        settle(w[t].at[0:3], send.at[t, 1])
        settle(w[t].at[0, 0:3], send.at[t, 2])
        settle(w[t].at[0, 0, 0:3], send.at[t, 3])
        settle(w[t].at[0, 0, 0:3], send.at[t, 4])
        settle(w[t].at[0, 0:3], send.at[t, 5])
        settle(w[t].at[0:3], send.at[t, 6])
        settle(w[t], send.at[t, 7])
        settle(w[t].at[0, 0, 0:3], send.at[t, 8])
        settle(w[t].at[0, 0:3], send.at[t, 9])
        settle(other[t], recv.at[t, GC])
    settle(px, xs.at[0])
    settle(st1.at[0:7], t1s.at[0])
    settle(st2.at[0:15], t2s.at[0])
    settle(rb.at[0:15], t3s.at[0])


def layout_kernel(*refs):
    own, other = refs[0:3], refs[3:6]
    newp, rown, coln = refs[6:9]
    whole, newp_out, rown_out, coln_out, sems = refs[9:]
    _, _, _, core = where_am_i()
    for src, dst in ((newp, newp_out), (rown, rown_out), (coln, coln_out)):
        pltpu.make_async_copy(src, dst, sems.at[3]).start()
    for held, c in ((own, core), (other, 1 - core)):
        for t in range(3):
            for a1 in range(4):
                for dst, src in copies(t, a1, c, whole, held[t]):
                    pltpu.make_async_copy(src, dst, sems.at[t]).start()
    for t in range(3):
        for held in (own, other):
            pltpu.make_async_copy(held[t], held[t], sems.at[t]).wait()
    for src, dst in ((newp, newp_out), (rown, rown_out), (coln, coln_out)):
        pltpu.make_async_copy(src, dst, sems.at[3]).wait()


def solution(mesh):
    block = [(r, 128) for r in ROWS]
    part = [jax.ShapeDtypeStruct((4, 4, 4) + b, BF16) for b in block]
    vmem = pl.BlockSpec(memory_space=pltpu.VMEM)
    anywhere = pl.BlockSpec(memory_space=pl.ANY)

    def hbm(v):
        return pltpu.with_memory_space_constraint(v, pltpu.HBM)

    def local(grad_bucket, parameters, row_state, column_state):
        def three(*lead, dtype=BF16):
            return [pltpu.VMEM(lead + b, dtype) for b in block]

        scratch = (
            three(4, 4, 4) + three(4, 4, 4) + three(4, 2) + three(4, 2) + three(4, 4) + three(4, 4) + three(4, 4)
            + three(3, 4) + three(3) + three(3) + three(dtype=F32) + three(4, 4) + three(4, 4)
            + [
                pltpu.VMEM((28, KW), BF16), pltpu.VMEM((1, 28), F32), pltpu.VMEM((8, 128), F32), pltpu.VMEM((8, 128), F32),
                pltpu.VMEM((56, 1024), F32),
                pltpu.VMEM((56, 512), BF16), pltpu.VMEM((56, 512), BF16),
                pltpu.VMEM((8, 8, 128), F32), pltpu.VMEM((16, 8, 128), F32), pltpu.VMEM((16, 8, 128), F32),
                pltpu.VMEM((8, 8, 128), F32), pltpu.VMEM((8, 8, 128), F32), pltpu.VMEM((8, 128), F32),
                pltpu.SemaphoreType.DMA((3, NRECV)), pltpu.SemaphoreType.DMA((3, NSEND)),
                pltpu.SemaphoreType.DMA((1,)), pltpu.SemaphoreType.DMA((1,)),
                pltpu.SemaphoreType.DMA((7,)), pltpu.SemaphoreType.DMA((1,)),
                pltpu.SemaphoreType.DMA((15,)), pltpu.SemaphoreType.DMA((1,)),
                pltpu.SemaphoreType.DMA((15,)), pltpu.SemaphoreType.DMA((1,)),
                pltpu.SemaphoreType.DMA((3,)),
            ]
        )
        small = [
            jax.ShapeDtypeStruct((28, KW), BF16),
            jax.ShapeDtypeStruct((1, 28), F32),
            jax.ShapeDtypeStruct((8, 128), F32),
        ]
        held = pl.pallas_call(
            step_kernel,
            out_shape=part + part + small,
            in_specs=[pl.BlockSpec(memory_space=pltpu.HBM)] * 4,
            out_specs=[vmem] * 9,
            scratch_shapes=scratch,
            compiler_params=pltpu.CompilerParams(
                collective_id=0, has_side_effects=True, vmem_limit_bytes=40 * 1024 * 1024
            ),
            name="adafactor_step",
        )(
            grad_bucket.reshape(4, 2, 2, 4, 56, KW),
            hbm(parameters.reshape(28, KW)),
            hbm(row_state),
            hbm(column_state.reshape(8, 128)),
        )
        whole, newp, rown, coln = pl.pallas_call(
            layout_kernel,
            out_shape=[jax.ShapeDtypeStruct((4, 2, 2, 4, 56, KW), BF16)] + small,
            in_specs=[vmem] * 9,
            out_specs=[anywhere] * 4,
            scratch_shapes=[pltpu.SemaphoreType.DMA((4,))],
            compiler_params=pltpu.CompilerParams(vmem_limit_bytes=20 * 1024 * 1024),
            name="lay_out",
        )(*held)
        return newp.reshape(1, 28, KW), rown, coln.reshape(1, KW), whole.reshape(D, KW)

    every = ("gx", "gy", "gz")
    return jax.shard_map(
        local,
        mesh=mesh,
        in_specs=(P(every, None, None, None), P(None, every, None), P(None, every), P(None, None)),
        out_specs=(P(None, every, None), P(None, every), P(None, None), P(None, None)),
        check_vma=False,
    )
```
